128 devices in a mesh: blk: 128 (over y, z, x, core).
Axes of the slice: x: 4, y: 4, z: 4, core: 2. Of those that a mesh axis runs over, the one named last changes fastest.
Arguments:
- defect: float32 [1536, 128], P('blk'), may hold values from -6 to 6
- mass: float32 [1536, 128], P('blk'), may hold values from 1 to 2
- block_diag: float32 [1536, 128, 128], P('blk'), may hold values from -0.1875 to 0.1875
- coupling: float32 [12288, 128, 128], P('blk'), may hold values from -0.09375 to 0.09375
- tile_rows: int32 [12288], P('blk'), may hold values from 0 to 1535, as said below
- tile_cols: int32 [12288], P('blk'), may hold values from 0 to 1535, as said below
Outputs:
- update: float32 [1536, 128], P('blk')
The draws below stay inside these ranges and needn't reach their ends.
Inputs may be any that keep to these rules, and one draw needn't show every extreme that they name: `tile_rows`: block rows d * 12 to d * 12 + 11 belong to device d of blk, and each device holds the tiles at positions d * 96 to d * 96 + 95. Of every tile a device holds, exactly one of its block row and block column belongs to that device; the other belongs to a different device. Exactly half of the 96 tiles of every device have their block row with that device, and the other half their block column. A program may send only the blocks and products of tiles that exist; slots of a padded buffer that no tile fills need not be sent. `tile_cols`: of one device's tiles, at most 1 have their block column with any one other device and at most 1 have their block row with any one other device; every device reaches 1 with some other device on each of the two sides.
All inputs are finite; a program needn't handle non-finite values.
Results may differ from the reference program's by a relative error of at most 0.0001.
Values sent between devices are 32-bit elements; how exact they have to be, the bound alone decides.
A program may use at most 64 MiB of HBM per device.

```python
import jax
import jax.numpy as jnp
from jax import lax

B = 128
K = 8
RB = 12
ITERS = 3
TD = 96
C = 1
NB = 1536
NT = 12288
N_BLK = 128


def tile_pattern(key):
    base = jax.random.fold_in(key, 11)
    half = TD // 2
    peers = N_BLK - 1
    cells = peers * C
    antipode_lane = N_BLK // 2 - 1

    def one_device(device_key, device):
        keys = jax.random.split(device_key, 6)

        def pick(pick_key):
            order = jax.random.permutation(pick_key, cells).astype(jnp.int32)
            grid = jnp.arange(cells, dtype=jnp.int32)
            score = jnp.where(grid // C == antipode_lane, grid - cells, order)
            return (jnp.argsort(score, stable=True)[:half] // C).astype(jnp.int32)
        lanes = jnp.concatenate([pick(keys[1]), pick(keys[2])])
        far_device = (device + lanes + 1) % N_BLK
        own_slot = jax.random.randint(keys[3], (TD,), 0, RB).astype(jnp.int32)
        far_slot = jax.random.randint(keys[4], (TD,), 0, RB).astype(jnp.int32)
        own_block = device * RB + own_slot
        far_block = far_device * RB + far_slot
        first = jnp.arange(TD) < half
        rows = jnp.where(first, own_block, far_block)
        cols = jnp.where(first, far_block, own_block)
        shuffle = jax.random.permutation(keys[5], TD)
        return (rows[shuffle], cols[shuffle])
    owners = jnp.arange(N_BLK, dtype=jnp.int32)
    rows, cols = jax.vmap(one_device)(jax.random.split(base, N_BLK), owners)
    return (rows.reshape(NT).astype(jnp.int32), cols.reshape(NT).astype(jnp.int32))


def draw_tile_rows(key, part):
    return tile_pattern(key)[0]


def draw_tile_cols(key, part):
    return tile_pattern(key)[1]


def levels(rng, dims, cuts, least, top_value):
    def one(axis_at, blocks):
        steps = jax.random.uniform(jax.random.fold_in(jax.random.fold_in(rng, 6), axis_at), (blocks,), jnp.float32, least / len(cuts), top_value / len(cuts))
        return jnp.repeat(jnp.exp(steps), dims[axis_at] // blocks).reshape((-1,) + (1,) * (len(dims) - axis_at - 1))

    loudness = one(*cuts[0])
    for cut in cuts[1:]:
        loudness = loudness * one(*cut)
    return loudness


def gaussian(key, shape, scale, limit, cuts=(), held_as=jnp.bfloat16):
    drawn = jax.random.normal(key, shape, jnp.float32) * scale
    if len(cuts) > 0:
        drawn = levels(key, shape, cuts, -0.22, 0.18) * drawn
    return jnp.clip(drawn, min=-limit, max=limit).astype(held_as)


def setup_inputs(seed: int = 0) -> dict:
    splits = jax.random.split(jax.random.key(seed), 7)
    return {
        "defect": gaussian(splits[0], (NB, B), 1.0, 6.0, ((0, 128),), jnp.float32),
        "mass": jnp.clip(1.0 + 1.0 * jax.random.uniform(splits[1], (NB, B), jnp.float32) ** levels(splits[1], (NB, B), ((0, 128),), -0.2, 0.2), 1.0, 2.0),
        "block_diag": gaussian(splits[2], (NB, B, B), (8 * B) ** -0.5, 0.1875, ((0, 128),), jnp.float32),
        "coupling": gaussian(splits[3], (NT, B, B), (4 * K * B) ** -0.5, 0.09375, ((0, 128),), jnp.float32),
        "tile_rows": draw_tile_rows(jax.random.fold_in(splits[6], 71), 0),
        "tile_cols": draw_tile_cols(jax.random.fold_in(splits[6], 71), 0),
    }


def solve_small(gram, target):
    factor = jnp.linalg.cholesky(gram)
    count = gram.shape[0]
    forward = []
    for index in range(count):
        value = target[index]
        for inner in range(index):
            value = value - factor[index, inner] * forward[inner]
        forward.append(value / factor[index, index])
    backward = [None] * count
    for index in reversed(range(count)):
        value = forward[index]
        for inner in range(index + 1, count):
            value = value - factor[inner, index] * backward[inner]
        backward[index] = value / factor[index, index]
    return backward

def newton_apply(vector, mass, block_diag, coupling, tile_rows, tile_cols):
    own = jnp.einsum('rij,rj->ri', block_diag, vector, precision=lax.Precision.HIGHEST)
    products = jnp.einsum('tij,tj->ti', coupling, vector[tile_cols], precision=lax.Precision.HIGHEST)
    far = jax.ops.segment_sum(products, tile_rows, num_segments=NB)
    return mass * vector + own + far

def reference(defect, mass, block_diag, coupling, tile_rows, tile_cols):
    negated = -defect
    beta = jnp.sqrt(jnp.sum(negated * negated))
    basis = [negated / beta]
    upper = jnp.zeros((ITERS + 1, ITERS), jnp.float32)
    for column in range(ITERS):
        image = newton_apply(basis[column], mass, block_diag, coupling, tile_rows, tile_cols)
        dots = jnp.stack([jnp.sum(item * image) for item in basis])
        for index in range(column + 1):
            image = image - dots[index] * basis[index]
        norm = jnp.sqrt(jnp.sum(image * image))
        upper = upper.at[:column + 1, column].set(dots)
        upper = upper.at[column + 1, column].set(norm)
        if column + 1 < ITERS:
            basis.append(image / norm)
    gram = jnp.dot(upper.T.astype(jnp.float32), upper.astype(jnp.float32), precision=lax.Precision.HIGHEST, preferred_element_type=jnp.float32)
    mixing = solve_small(gram, beta * upper[0, :])
    update = jnp.zeros_like(defect)
    for index in range(ITERS):
        update = update + mixing[index] * basis[index]
    return update
```

```python
import itertools

import jax
import jax.numpy as jnp
from jax import lax
from jax.experimental import pallas as pl
from jax.experimental.pallas import tpu as pltpu
from jax.sharding import PartitionSpec as P

N = 128
RB = 12
TD = 96
HALF = 48
B = 128
SHIFT = 1.5
F32 = jnp.float32
BF16 = jnp.bfloat16
MESH = pl.DeviceIdType.MESH


def distance(offset):
    return sum(min(step, 4 - step) for step in offset[:3]) + 0.5 * offset[3]


OFFSETS = sorted(
    (o for o in itertools.product(range(4), range(4), range(4), range(2)) if any(o)),
    key=distance,
    reverse=True,
)


def dot(a, b):
    return lax.dot_general(a, b, (((1,), (0,)), ((), ())), preferred_element_type=F32)


def dot_nt(a, b):
    return lax.dot_general(a, b, (((1,), (1,)), ((), ())), preferred_element_type=F32)


def iota(shape, dim):
    return lax.broadcasted_iota(jnp.int32, shape, dim)


def halves(x):
    high = x.astype(BF16)
    low = (x - high.astype(F32)).astype(BF16)
    return high, low


def total(x):
    return jnp.sum(jnp.sum(x, axis=0, keepdims=True), axis=1, keepdims=True)


def divided_by_rb(x):
    return lax.shift_right_logical(x * 21846, 18)


def kernel(
    defect_ref, mass_ref, diag_hbm, coup_hbm, rows_ref, cols_ref, out_ref,
    raw, raw_diag, weights, index_rows, perm_vmem, perm_smem,
    ysplit, products, oh_fetch_out, oh_push_in, oh_cols, oh_push_out, oh_local, oh_fetch_in,
    req_out, req_in, x_out, x_in, p_out, p_in, f_out, f_in,
    load_sem, perm_sem, send_sem, recv_sem,
):
    me = lax.axis_index("blk")
    y, z, x, c = me // 32, (me // 8) % 4, (me // 2) % 4, me % 2
    y_part = [((y + d) % 4) * 32 for d in range(4)]
    z_part = [((z + d) % 4) * 8 for d in range(4)]
    x_part = [((x + d) % 4) * 2 for d in range(4)]
    c_part = [(c + d) % 2 for d in range(2)]
    yz = [[y_part[a] + z_part[b] for b in range(4)] for a in range(4)]
    xc = [[x_part[a] + c_part[b] for b in range(2)] for a in range(4)]
    peers = [yz[o[0]][o[1]] + xc[o[2]][o[3]] for o in OFFSETS]

    req_in[...] = jnp.zeros_like(req_in)
    x_in[...] = jnp.zeros_like(x_in)
    p_in[...] = jnp.zeros_like(p_in)
    f_in[...] = jnp.zeros_like(f_in)

    barrier = pltpu.get_barrier_semaphore()
    for peer in peers:
        pl.semaphore_signal(barrier, inc=1, device_id=(peer,), device_id_type=MESH)

    loads = [
        pltpu.make_async_copy(
            coup_hbm.at[pl.ds(16 * i, 16)], raw.at[pl.ds(16 * i, 16)], load_sem.at[i]
        )
        for i in range(6)
    ]
    loads.append(pltpu.make_async_copy(diag_hbm, raw_diag, load_sem.at[6]))
    for load in loads:
        load.start()

    lane_row = iota((1, B), 1)
    lanes = iota((B, B), 1)
    subs = iota((B, B), 0)
    index_rows[...] = jnp.zeros_like(index_rows)
    index_rows[0:1, 0:TD] = rows_ref[...]
    index_rows[1:2, 0:TD] = cols_ref[...]
    rows = index_rows[0:1, :]
    cols = index_rows[1:2, :]
    row_owner = divided_by_rb(rows)
    col_owner = divided_by_rb(cols)
    row_local = rows - row_owner * RB
    col_local = cols - col_owner * RB
    valid = lane_row < TD
    push = valid & (row_owner != me)
    fetch = valid & (row_owner == me)
    push_f = jnp.where(push, 1.0, 0.0)
    fetch_f = jnp.where(fetch, 1.0, 0.0)
    sub8 = iota((16, B), 0)
    both = jnp.where(sub8 == 0, push_f, jnp.where(sub8 == 1, fetch_f, 0.0))
    ranks = dot(both.astype(BF16), jnp.where(subs < lanes, 1.0, 0.0).astype(BF16))
    position = jnp.where(
        push, ranks[0:1], jnp.where(fetch, ranks[1:2] + HALF, 1000.0)
    ).astype(jnp.int32)
    order = jnp.where(position == subs, 1.0, 0.0).astype(BF16)

    def as_f(v):
        return v.astype(F32)

    destination = jnp.where(push, row_owner, col_owner)
    wanted = jnp.where(fetch, as_f(col_local) + 1.0, 0.0)
    target = jnp.where(push, as_f(row_local) + 1.0, 0.0)
    table = jnp.zeros((B, B), F32)
    for at, value in enumerate(
        (wanted, target, as_f(destination), as_f(col_local), as_f(row_local), as_f(lane_row))
    ):
        table = jnp.where(subs == at, value, table)
    table = table.astype(BF16)
    by_lane = dot_nt(table, order)
    by_sub = dot_nt(order, table)
    dest_lane = by_lane[2:3].astype(jnp.int32)
    row_local_lane = by_lane[4:5].astype(jnp.int32)
    perm_vmem[...] = by_lane[5:6].astype(jnp.int32)
    to_smem = pltpu.make_async_copy(perm_vmem, perm_smem, perm_sem)
    to_smem.start()

    sends_to = jnp.where((dest_lane == subs) & (lanes < TD), 1.0, 0.0)
    push_out = jnp.where(lanes < HALF, sends_to, 0.0).astype(BF16)
    oh_push_out[:, 0:B] = push_out
    oh_push_out[:, B:] = push_out
    dest_sub = by_sub[HALF:TD, 2:3].astype(jnp.int32)
    oh_fetch_in[...] = jnp.where(dest_sub == lanes[0:HALF], 1.0, 0.0).astype(BF16)
    col_local_sub = by_sub[0:HALF, 3:4].astype(jnp.int32)
    oh_cols[...] = jnp.where(col_local_sub == iota((HALF, 16), 1), 1.0, 0.0).astype(BF16)
    lanes16 = iota((16, B), 1)
    local_target = jnp.where(
        (lanes16 >= HALF) & (lanes16 < TD),
        row_local_lane,
        jnp.where((lanes16 >= TD) & (lanes16 < TD + RB), lanes16 - TD, -1),
    )
    local = jnp.where(local_target == sub8, 1.0, 0.0).astype(BF16)
    oh_local[:, 0:B] = local
    oh_local[:, B:] = local

    ysplit[...] = jnp.zeros_like(ysplit)
    products[...] = jnp.zeros_like(products)
    zeros4 = jnp.zeros((4, B), F32)
    u0 = jnp.concatenate([-defect_ref[...], zeros4], axis=0)
    mass = jnp.concatenate([mass_ref[...] - SHIFT, zeros4], axis=0)
    beta_part = total(u0 * u0)
    message = dot(sends_to.astype(BF16), by_sub.astype(BF16))
    req_out[...] = jnp.where(lanes < 2, message, jnp.where(lanes == 2, beta_part, 0.0))

    pl.semaphore_wait(barrier, N - 1)

    def send(source, landing, at):
        for peer in peers:
            pltpu.make_async_remote_copy(
                src_ref=source(peer), dst_ref=landing(me),
                send_sem=send_sem.at[at], recv_sem=recv_sem.at[at],
                device_id=(peer,), device_id_type=MESH,
            ).start()

    def received(ref, at):
        pltpu.make_async_copy(ref, ref, recv_sem.at[at]).wait()

    def sent(ref, at):
        pltpu.make_async_copy(ref, ref, send_sem.at[at]).wait()

    one_row = pl.ds(0, N - 1)
    send(lambda p: req_out.at[pl.ds(p, 1)], lambda m: req_in.at[pl.ds(m, 1)], 0)

    for load in loads:
        load.wait()
    to_smem.wait()

    def put(pair, tile, at):
        high, low = halves(tile.T)
        weights[pair, 0:B, at * B : (at + 1) * B] = high
        weights[pair, B:, at * B : (at + 1) * B] = low

    def in_order(at):
        return raw[jnp.minimum(jnp.maximum(perm_smem[0, at], 0), TD - 1)]

    def prepare(pair, carry):
        put(pair, in_order(2 * pair), 0)
        put(pair, in_order(2 * pair + 1), 1)
        return carry

    lax.fori_loop(0, HALF, prepare, 0)

    def prepare_diag(pair, carry):
        put(HALF + pair, raw_diag[2 * pair], 0)
        put(HALF + pair, raw_diag[2 * pair + 1], 1)
        return carry

    lax.fori_loop(0, RB // 2, prepare_diag, 0)

    rows16 = iota((16, B), 0)

    def tile_products(high, low, first_pair, pairs):
        lhs = jnp.concatenate(
            [jnp.concatenate([high, high], axis=1), jnp.concatenate([low, low], axis=1)], axis=0
        )
        out = jnp.zeros((16, B), F32)
        for i in range(pairs):
            got = dot(lhs, weights[first_pair + i])
            got = got[0:16] + got[16:32]
            out = jnp.where(
                rows16 == 2 * i, got[:, 0:B], jnp.where(rows16 == 2 * i + 1, got[:, B:], out)
            )
        return out

    def push_products(high, low, at):
        picked = dot(oh_cols[...], jnp.concatenate([high, low], axis=1))
        picked = picked.astype(BF16)
        for b in range(3):
            block = picked[16 * b : 16 * b + 16]
            products[16 * b : 16 * b + 16] = tile_products(
                block[:, 0:B], block[:, B:], 8 * b, 8
            )
        p_high, p_low = halves(products[...])
        p_out[at] = dot(oh_push_out[...], jnp.concatenate([p_high, p_low], axis=0))
        send(
            lambda p: p_out.at[at, pl.ds(p, 1)], lambda m: p_in.at[at, pl.ds(m, 1)], 4 + at
        )

    def send_x(vector, high, low, dots_row, at):
        rest = (vector - high.astype(F32) - low.astype(F32)).astype(BF16)
        ysplit[0:16] = high
        ysplit[16:32] = low
        ysplit[32:48] = rest
        x_out[at, 0] = dot(oh_fetch_out[...], ysplit[...])
        x_out[at, 1] = jnp.broadcast_to(dots_row, (B, B))
        send(
            lambda p: x_out.at[at, :, pl.ds(p, 1)],
            lambda m: x_in.at[at, :, pl.ds(m, 1)],
            1 + at,
        )

    def finish(vector, high, low, at):
        products[TD : TD + 16] = tile_products(high, low, HALF, RB // 2)
        received(x_in.at[at, :, one_row], 1 + at)
        x_high, x_low = halves(x_in[at, 0])
        picked = dot(oh_fetch_in[...], jnp.concatenate([x_high, x_low], axis=1))
        picked = picked.astype(BF16)
        for b in range(3):
            block = picked[16 * b : 16 * b + 16]
            products[HALF + 16 * b : HALF + 16 * b + 16] = tile_products(
                block[:, 0:B], block[:, B:], 24 + 8 * b, 8
            )
        p_high, p_low = halves(products[...])
        here = mass * vector + dot(oh_local[...], jnp.concatenate([p_high, p_low], axis=0))
        received(p_in.at[at, one_row], 4 + at)
        p_high, p_low = halves(p_in[at])
        return here + dot(oh_push_in[...], jnp.concatenate([p_high, p_low], axis=0))

    def packed(values):
        row = jnp.zeros((1, B), F32)
        for i, value in enumerate(values):
            row = jnp.where(lane_row == i, value, row)
        return row

    def unpacked(row, count):
        return [
            jnp.sum(jnp.where(lane_row == i, row, 0.0), axis=1, keepdims=True)
            for i in range(count)
        ]

    u_high, u_low = halves(u0)
    push_products(u_high, u_low, 0)
    received(req_in.at[one_row], 0)
    req = req_in[...]
    slot = lanes % 16
    asked = req[:, 0:1].astype(jnp.int32) - 1
    oh_fetch_out[...] = jnp.where((asked == slot) & (lanes < 48), 1.0, 0.0).astype(BF16)
    send_x(u0, u_high, u_low, jnp.zeros((1, B), F32), 0)
    landing = req[:, 1:2].astype(jnp.int32) - 1
    into = jnp.where(landing == lanes, 1.0, 0.0).T[0:16].astype(BF16)
    oh_push_in[:, 0:B] = into
    oh_push_in[:, B:] = into
    beta_row = jnp.where(lane_row == 2, jnp.sum(req, axis=0, keepdims=True), 0.0)
    beta = jnp.sqrt(jnp.sum(beta_row, axis=1, keepdims=True) + beta_part)
    v0 = u0 / beta
    w0 = finish(u0, u_high, u_low, 0) / beta

    def apply_with_dots(vector, others, at):
        row = packed([total(other * vector) for other in others] + [total(vector * vector)])
        high, low = halves(vector)
        send_x(vector, high, low, row, at)
        push_products(high, low, at)
        image = finish(vector, high, low, at)
        sums = jnp.sum(x_in[at, 1], axis=0, keepdims=True) + row
        return image, unpacked(sums, len(others) + 1)

    z1, (h00, square) = apply_with_dots(w0, [v0], 1)
    h10 = jnp.sqrt(square - h00 * h00)
    v1 = (w0 - h00 * v0) / h10
    w1 = (z1 - h00 * w0) / h10

    z2, (h01, h11, square) = apply_with_dots(w1, [v0, v1], 2)
    h21 = jnp.sqrt(square - h01 * h01 - h11 * h11)
    v2 = (w1 - h01 * v0 - h11 * v1) / h21
    w2 = (z2 - h01 * w0 - h11 * w1) / h21

    row = packed([total(v0 * w2), total(v1 * w2), total(v2 * w2), total(w2 * w2)])
    f_out[...] = jnp.broadcast_to(row, (8, B))
    send(lambda p: f_out.at[pl.ds(0, 1)], lambda m: f_in.at[pl.ds(m, 1)], 7)
    received(f_in.at[one_row], 7)
    sums = jnp.sum(f_in[...], axis=0, keepdims=True) + row
    h02, h12, h22, square = unpacked(sums, 4)
    h32 = jnp.sqrt(square - h02 * h02 - h12 * h12 - h22 * h22)

    h00, h11, h22 = h00 + SHIFT, h11 + SHIFT, h22 + SHIFT
    g00 = h00 * h00 + h10 * h10
    g10 = h01 * h00 + h11 * h10
    g20 = h02 * h00 + h12 * h10
    g11 = h01 * h01 + h11 * h11 + h21 * h21
    g21 = h02 * h01 + h12 * h11 + h22 * h21
    g22 = h02 * h02 + h12 * h12 + h22 * h22 + h32 * h32
    l00 = jnp.sqrt(g00)
    l10, l20 = g10 / l00, g20 / l00
    l11 = jnp.sqrt(g11 - l10 * l10)
    l21 = (g21 - l20 * l10) / l11
    l22 = jnp.sqrt(g22 - l20 * l20 - l21 * l21)
    t0 = beta * h00 / l00
    t1 = (beta * h01 - l10 * t0) / l11
    t2 = (beta * h02 - l20 * t0 - l21 * t1) / l22
    m2 = t2 / l22
    m1 = (t1 - l21 * m2) / l11
    m0 = (t0 - l10 * m1 - l20 * m2) / l00
    update = m0 * v0 + m1 * v1 + m2 * v2
    out_ref[...] = update[0:RB]

    sent(req_out.at[one_row], 0)
    for at in range(3):
        sent(x_out.at[at, :, one_row], 1 + at)
        sent(p_out.at[at, one_row], 4 + at)
    sent(f_in.at[one_row], 7)


def on_device(defect, mass, block_diag, coupling, tile_rows, tile_cols):
    vmem = pl.BlockSpec(memory_space=pltpu.VMEM)
    hbm = pl.BlockSpec(memory_space=pl.ANY)
    return pl.pallas_call(
        kernel,
        out_shape=jax.ShapeDtypeStruct(defect.shape, F32),
        in_specs=[vmem, vmem, hbm, hbm, vmem, vmem],
        out_specs=vmem,
        scratch_shapes=[
            pltpu.VMEM((TD, B, B), F32),
            pltpu.VMEM((RB, B, B), F32),
            pltpu.VMEM((54, 2 * B, 2 * B), BF16),
            pltpu.VMEM((8, B), jnp.int32),
            pltpu.VMEM((1, B), jnp.int32),
            pltpu.SMEM((1, B), jnp.int32),
            pltpu.VMEM((B, B), BF16),
            pltpu.VMEM((B, B), F32),
            pltpu.VMEM((B, B), BF16),
            pltpu.VMEM((16, 2 * B), BF16),
            pltpu.VMEM((HALF, 16), BF16),
            pltpu.VMEM((B, 2 * B), BF16),
            pltpu.VMEM((16, 2 * B), BF16),
            pltpu.VMEM((HALF, B), BF16),
            pltpu.VMEM((N, B), F32),
            pltpu.VMEM((N, B), F32),
            pltpu.VMEM((3, 2, N, B), F32),
            pltpu.VMEM((3, 2, N, B), F32),
            pltpu.VMEM((3, N, B), F32),
            pltpu.VMEM((3, N, B), F32),
            pltpu.VMEM((8, B), F32),
            pltpu.VMEM((N, B), F32),
            pltpu.SemaphoreType.DMA((7,)),
            pltpu.SemaphoreType.DMA,
            pltpu.SemaphoreType.DMA((8,)),
            pltpu.SemaphoreType.DMA((8,)),
        ],
        compiler_params=pltpu.CompilerParams(collective_id=0, has_side_effects=True),
    )(
        defect, mass, block_diag, coupling,
        tile_rows.reshape(1, TD), tile_cols.reshape(1, TD),
    )


def solution(mesh):
    return jax.shard_map(
        on_device,
        mesh=mesh,
        in_specs=(
            P("blk", None),
            P("blk", None),
            P("blk", None, None),
            P("blk", None, None),
            P("blk"),
            P("blk"),
        ),
        out_specs=P("blk", None),
        check_vma=False,
    )
```

```python
import itertools

import jax
import jax.numpy as jnp
from jax import lax
from jax.experimental import pallas as pl
from jax.experimental.pallas import tpu as pltpu
from jax.sharding import PartitionSpec as P

N = 128
RB = 12
TD = 96
HALF = 48
B = 128
SHIFT = 1.5
F32 = jnp.float32
BF16 = jnp.bfloat16
MESH = pl.DeviceIdType.MESH


def distance(offset):
    return sum(min(step, 4 - step) for step in offset[:3]) + 0.5 * offset[3]


OFFSETS = sorted(
    (o for o in itertools.product(range(4), range(4), range(4), range(2)) if any(o)),
    key=distance,
    reverse=True,
)


def dot(a, b):
    return lax.dot_general(a, b, (((1,), (0,)), ((), ())), preferred_element_type=F32)


def dot_nt(a, b):
    return lax.dot_general(a, b, (((1,), (1,)), ((), ())), preferred_element_type=F32)


def iota(shape, dim):
    return lax.broadcasted_iota(jnp.int32, shape, dim)


def halves(x):
    high = x.astype(BF16)
    low = (x - high.astype(F32)).astype(BF16)
    return high, low


def total(x):
    return jnp.sum(jnp.sum(x, axis=0, keepdims=True), axis=1, keepdims=True)


def divided_by_rb(x):
    return lax.shift_right_logical(x * 21846, 18)


def kernel(
    defect_hbm, mass_hbm, diag_hbm, coup_hbm, rows_hbm, cols_hbm, out_ref,
    indices, vectors, raw, raw_diag, weights, index_rows, perm_vmem, perm_smem,
    ysplit, products, oh_fetch_out, oh_push_in, oh_cols, oh_push_out, oh_local, oh_fetch_in,
    req_out, req_in, x_out, x_in, p_out, p_in, f_out, f_in,
    load_sem, small_sem, perm_sem, send_sem, recv_sem,
):
    me = lax.axis_index("blk")
    y, z, x, c = me // 32, (me // 8) % 4, (me // 2) % 4, me % 2
    y_part = [((y + d) % 4) * 32 for d in range(4)]
    z_part = [((z + d) % 4) * 8 for d in range(4)]
    x_part = [((x + d) % 4) * 2 for d in range(4)]
    c_part = [(c + d) % 2 for d in range(2)]
    yz = [[y_part[a] + z_part[b] for b in range(4)] for a in range(4)]
    xc = [[x_part[a] + c_part[b] for b in range(2)] for a in range(4)]
    peers = [yz[o[0]][o[1]] + xc[o[2]][o[3]] for o in OFFSETS]

    mine = pl.ds(me, 1)
    nothing = jnp.zeros((1, B), F32)
    req_in[mine] = nothing
    f_in[mine] = nothing
    for at in range(3):
        x_in[at, 0, mine] = nothing
        x_in[at, 1, mine] = nothing
        p_in[at, mine] = nothing

    barrier = pltpu.get_barrier_semaphore()
    for peer in peers:
        pl.semaphore_signal(barrier, inc=1, device_id=(peer,), device_id_type=MESH)

    small_loads = [
        pltpu.make_async_copy(rows_hbm, indices.at[0], small_sem.at[0]),
        pltpu.make_async_copy(cols_hbm, indices.at[1], small_sem.at[1]),
        pltpu.make_async_copy(defect_hbm, vectors.at[0, 0:RB], small_sem.at[2]),
        pltpu.make_async_copy(mass_hbm, vectors.at[1, 0:RB], small_sem.at[3]),
    ]
    for load in small_loads:
        load.start()
    loads = [
        pltpu.make_async_copy(
            coup_hbm.at[pl.ds(16 * i, 16)], raw.at[pl.ds(16 * i, 16)], load_sem.at[i]
        )
        for i in range(6)
    ]
    loads.append(pltpu.make_async_copy(diag_hbm, raw_diag, load_sem.at[6]))
    for load in loads:
        load.start()

    lane_row = iota((1, B), 1)
    lanes = iota((B, B), 1)
    subs = iota((B, B), 0)
    ysplit[...] = jnp.zeros_like(ysplit)
    products[...] = jnp.zeros_like(products)
    for load in small_loads:
        load.wait()
    index_rows[...] = jnp.zeros_like(index_rows)
    index_rows[0:1, 0:TD] = indices[0]
    index_rows[1:2, 0:TD] = indices[1]
    rows = index_rows[0:1, :]
    cols = index_rows[1:2, :]
    row_owner = divided_by_rb(rows)
    col_owner = divided_by_rb(cols)
    row_local = rows - row_owner * RB
    col_local = cols - col_owner * RB
    valid = lane_row < TD
    push = valid & (row_owner != me)
    fetch = valid & (row_owner == me)
    push_f = jnp.where(push, 1.0, 0.0)
    fetch_f = jnp.where(fetch, 1.0, 0.0)
    sub8 = iota((16, B), 0)
    both = jnp.where(sub8 == 0, push_f, jnp.where(sub8 == 1, fetch_f, 0.0))
    ranks = dot(both.astype(BF16), jnp.where(subs < lanes, 1.0, 0.0).astype(BF16))
    position = jnp.where(
        push, ranks[0:1], jnp.where(fetch, ranks[1:2] + HALF, 1000.0)
    ).astype(jnp.int32)
    order = jnp.where(position == subs, 1.0, 0.0).astype(BF16)

    def as_f(v):
        return v.astype(F32)

    destination = jnp.where(push, row_owner, col_owner)
    wanted = jnp.where(fetch, as_f(col_local) + 1.0, 0.0)
    target = jnp.where(push, as_f(row_local) + 1.0, 0.0)
    table = jnp.zeros((B, B), F32)
    for at, value in enumerate(
        (wanted, target, as_f(destination), as_f(col_local), as_f(row_local), as_f(lane_row))
    ):
        table = jnp.where(subs == at, value, table)
    table = table.astype(BF16)
    by_lane = dot_nt(table, order)
    by_sub = dot_nt(order, table)
    dest_lane = by_lane[2:3].astype(jnp.int32)
    row_local_lane = by_lane[4:5].astype(jnp.int32)
    perm_vmem[...] = by_lane[5:6].astype(jnp.int32)
    to_smem = pltpu.make_async_copy(perm_vmem, perm_smem, perm_sem)
    to_smem.start()

    sends_to = jnp.where((dest_lane == subs) & (lanes < TD), 1.0, 0.0)
    push_out = jnp.where(lanes < HALF, sends_to, 0.0).astype(BF16)
    oh_push_out[:, 0:B] = push_out
    oh_push_out[:, B:] = push_out
    dest_sub = by_sub[HALF:TD, 2:3].astype(jnp.int32)
    oh_fetch_in[...] = jnp.where(dest_sub == lanes[0:HALF], 1.0, 0.0).astype(BF16)
    col_local_sub = by_sub[0:HALF, 3:4].astype(jnp.int32)
    oh_cols[...] = jnp.where(col_local_sub == iota((HALF, 16), 1), 1.0, 0.0).astype(BF16)
    lanes16 = iota((16, B), 1)
    local_target = jnp.where(
        (lanes16 >= HALF) & (lanes16 < TD),
        row_local_lane,
        jnp.where((lanes16 >= TD) & (lanes16 < TD + RB), lanes16 - TD, -1),
    )
    local = jnp.where(local_target == sub8, 1.0, 0.0).astype(BF16)
    oh_local[:, 0:B] = local
    oh_local[:, B:] = local

    own_rows = iota((16, B), 0) < RB
    u0 = jnp.where(own_rows, -vectors[0], 0.0)
    mass = jnp.where(own_rows, vectors[1] - SHIFT, 0.0)
    beta_part = total(u0 * u0)
    message = dot(sends_to.astype(BF16), by_sub.astype(BF16))
    req_out[...] = jnp.where(lanes < 2, message, jnp.where(lanes == 2, beta_part, 0.0))

    pl.semaphore_wait(barrier, N - 1)

    def send(source, landing, at):
        for peer in peers:
            pltpu.make_async_remote_copy(
                src_ref=source(peer), dst_ref=landing(me),
                send_sem=send_sem.at[at], recv_sem=recv_sem.at[at],
                device_id=(peer,), device_id_type=MESH,
            ).start()

    def received(ref, at):
        pltpu.make_async_copy(ref, ref, recv_sem.at[at]).wait()

    def sent(ref, at):
        pltpu.make_async_copy(ref, ref, send_sem.at[at]).wait()

    one_row = pl.ds(0, N - 1)
    send(lambda p: req_out.at[pl.ds(p, 1)], lambda m: req_in.at[pl.ds(m, 1)], 0)

    for load in loads:
        load.wait()
    to_smem.wait()

    def put(pair, tile, at):
        high, low = halves(tile.T)
        weights[pair, 0:B, at * B : (at + 1) * B] = high
        weights[pair, B:, at * B : (at + 1) * B] = low

    def in_order(at):
        return raw[jnp.minimum(jnp.maximum(perm_smem[0, at], 0), TD - 1)]

    for pair in range(HALF):
        put(pair, in_order(2 * pair), 0)
        put(pair, in_order(2 * pair + 1), 1)
    for pair in range(RB // 2):
        put(HALF + pair, raw_diag[2 * pair], 0)
        put(HALF + pair, raw_diag[2 * pair + 1], 1)

    rows16 = iota((16, B), 0)

    def tile_products(high, low, first_pair, pairs):
        lhs = jnp.concatenate(
            [jnp.concatenate([high, high], axis=1), jnp.concatenate([low, low], axis=1)], axis=0
        )
        out = jnp.zeros((16, B), F32)
        for i in range(pairs):
            got = dot(lhs, weights[first_pair + i])
            got = got[0:16] + got[16:32]
            out = jnp.where(
                rows16 == 2 * i, got[:, 0:B], jnp.where(rows16 == 2 * i + 1, got[:, B:], out)
            )
        return out

    def push_products(high, low, at):
        picked = dot(oh_cols[...], jnp.concatenate([high, low], axis=1))
        picked = picked.astype(BF16)
        for b in range(3):
            block = picked[16 * b : 16 * b + 16]
            products[16 * b : 16 * b + 16] = tile_products(
                block[:, 0:B], block[:, B:], 8 * b, 8
            )
        p_high, p_low = halves(products[...])
        p_out[at] = dot(oh_push_out[...], jnp.concatenate([p_high, p_low], axis=0))
        send(
            lambda p: p_out.at[at, pl.ds(p, 1)], lambda m: p_in.at[at, pl.ds(m, 1)], 4 + at
        )

    def send_x(vector, high, low, dots_row, at):
        rest = (vector - high.astype(F32) - low.astype(F32)).astype(BF16)
        ysplit[0:16] = high
        ysplit[16:32] = low
        ysplit[32:48] = rest
        x_out[at, 0] = dot(oh_fetch_out[...], ysplit[...])
        x_out[at, 1] = jnp.broadcast_to(dots_row, (B, B))
        send(
            lambda p: x_out.at[at, :, pl.ds(p, 1)],
            lambda m: x_in.at[at, :, pl.ds(m, 1)],
            1 + at,
        )

    def finish(vector, high, low, at):
        products[TD : TD + 16] = tile_products(high, low, HALF, RB // 2)
        received(x_in.at[at, :, one_row], 1 + at)
        x_high, x_low = halves(x_in[at, 0])
        picked = dot(oh_fetch_in[...], jnp.concatenate([x_high, x_low], axis=1))
        picked = picked.astype(BF16)
        for b in range(3):
            block = picked[16 * b : 16 * b + 16]
            products[HALF + 16 * b : HALF + 16 * b + 16] = tile_products(
                block[:, 0:B], block[:, B:], 24 + 8 * b, 8
            )
        p_high, p_low = halves(products[...])
        here = mass * vector + dot(oh_local[...], jnp.concatenate([p_high, p_low], axis=0))
        received(p_in.at[at, one_row], 4 + at)
        p_high, p_low = halves(p_in[at])
        return here + dot(oh_push_in[...], jnp.concatenate([p_high, p_low], axis=0))

    def packed(values):
        row = jnp.zeros((1, B), F32)
        for i, value in enumerate(values):
            row = jnp.where(lane_row == i, value, row)
        return row

    def unpacked(row, count):
        return [
            jnp.sum(jnp.where(lane_row == i, row, 0.0), axis=1, keepdims=True)
            for i in range(count)
        ]

    u_high, u_low = halves(u0)
    push_products(u_high, u_low, 0)
    received(req_in.at[one_row], 0)
    req = req_in[...]
    slot = lanes % 16
    asked = req[:, 0:1].astype(jnp.int32) - 1
    oh_fetch_out[...] = jnp.where((asked == slot) & (lanes < 48), 1.0, 0.0).astype(BF16)
    send_x(u0, u_high, u_low, jnp.zeros((1, B), F32), 0)
    landing = req[:, 1:2].astype(jnp.int32) - 1
    into = jnp.where(landing == lanes, 1.0, 0.0).T[0:16].astype(BF16)
    oh_push_in[:, 0:B] = into
    oh_push_in[:, B:] = into
    beta_row = jnp.where(lane_row == 2, jnp.sum(req, axis=0, keepdims=True), 0.0)
    beta = jnp.sqrt(jnp.sum(beta_row, axis=1, keepdims=True) + beta_part)
    v0 = u0 / beta
    w0 = finish(u0, u_high, u_low, 0) / beta

    def apply_with_dots(vector, others, at):
        row = packed([total(other * vector) for other in others] + [total(vector * vector)])
        high, low = halves(vector)
        send_x(vector, high, low, row, at)
        push_products(high, low, at)
        image = finish(vector, high, low, at)
        sums = jnp.sum(x_in[at, 1], axis=0, keepdims=True) + row
        return image, unpacked(sums, len(others) + 1)

    z1, (h00, square) = apply_with_dots(w0, [v0], 1)
    h10 = jnp.sqrt(square - h00 * h00)
    v1 = (w0 - h00 * v0) / h10
    w1 = (z1 - h00 * w0) / h10

    z2, (h01, h11, square) = apply_with_dots(w1, [v0, v1], 2)
    h21 = jnp.sqrt(square - h01 * h01 - h11 * h11)
    v2 = (w1 - h01 * v0 - h11 * v1) / h21
    w2 = (z2 - h01 * w0 - h11 * w1) / h21

    row = packed([total(v0 * w2), total(v1 * w2), total(v2 * w2), total(w2 * w2)])
    f_out[...] = jnp.broadcast_to(row, (8, B))
    send(lambda p: f_out.at[pl.ds(0, 1)], lambda m: f_in.at[pl.ds(m, 1)], 7)
    received(f_in.at[one_row], 7)
    sums = jnp.sum(f_in[...], axis=0, keepdims=True) + row
    h02, h12, h22, square = unpacked(sums, 4)
    h32 = jnp.sqrt(square - h02 * h02 - h12 * h12 - h22 * h22)

    h00, h11, h22 = h00 + SHIFT, h11 + SHIFT, h22 + SHIFT
    g00 = h00 * h00 + h10 * h10
    g10 = h01 * h00 + h11 * h10
    g20 = h02 * h00 + h12 * h10
    g11 = h01 * h01 + h11 * h11 + h21 * h21
    g21 = h02 * h01 + h12 * h11 + h22 * h21
    g22 = h02 * h02 + h12 * h12 + h22 * h22 + h32 * h32
    l00 = jnp.sqrt(g00)
    l10, l20 = g10 / l00, g20 / l00
    l11 = jnp.sqrt(g11 - l10 * l10)
    l21 = (g21 - l20 * l10) / l11
    l22 = jnp.sqrt(g22 - l20 * l20 - l21 * l21)
    t0 = beta * h00 / l00
    t1 = (beta * h01 - l10 * t0) / l11
    t2 = (beta * h02 - l20 * t0 - l21 * t1) / l22
    m2 = t2 / l22
    m1 = (t1 - l21 * m2) / l11
    m0 = (t0 - l10 * m1 - l20 * m2) / l00
    update = m0 * v0 + m1 * v1 + m2 * v2
    out_ref[...] = update[0:RB]

    sent(req_out.at[one_row], 0)
    for at in range(3):
        sent(x_out.at[at, :, one_row], 1 + at)
        sent(p_out.at[at, one_row], 4 + at)
    sent(f_in.at[one_row], 7)


def on_device(defect, mass, block_diag, coupling, tile_rows, tile_cols):
    vmem = pl.BlockSpec(memory_space=pltpu.VMEM)
    hbm = pl.BlockSpec(memory_space=pl.ANY)
    return pl.pallas_call(
        kernel,
        out_shape=pltpu.VMEM(defect.shape, F32),
        in_specs=[hbm] * 6,
        out_specs=vmem,
        scratch_shapes=[
            pltpu.VMEM((2, 1, TD), jnp.int32),
            pltpu.VMEM((2, 16, B), F32),
            pltpu.VMEM((TD, B, B), F32),
            pltpu.VMEM((RB, B, B), F32),
            pltpu.VMEM((54, 2 * B, 2 * B), BF16),
            pltpu.VMEM((8, B), jnp.int32),
            pltpu.VMEM((1, B), jnp.int32),
            pltpu.SMEM((1, B), jnp.int32),
            pltpu.VMEM((B, B), BF16),
            pltpu.VMEM((B, B), F32),
            pltpu.VMEM((B, B), BF16),
            pltpu.VMEM((16, 2 * B), BF16),
            pltpu.VMEM((HALF, 16), BF16),
            pltpu.VMEM((B, 2 * B), BF16),
            pltpu.VMEM((16, 2 * B), BF16),
            pltpu.VMEM((HALF, B), BF16),
            pltpu.VMEM((N, B), F32),
            pltpu.VMEM((N, B), F32),
            pltpu.VMEM((3, 2, N, B), F32),
            pltpu.VMEM((3, 2, N, B), F32),
            pltpu.VMEM((3, N, B), F32),
            pltpu.VMEM((3, N, B), F32),
            pltpu.VMEM((8, B), F32),
            pltpu.VMEM((N, B), F32),
            pltpu.SemaphoreType.DMA((7,)),
            pltpu.SemaphoreType.DMA((4,)),
            pltpu.SemaphoreType.DMA,
            pltpu.SemaphoreType.DMA((8,)),
            pltpu.SemaphoreType.DMA((8,)),
        ],
        compiler_params=pltpu.CompilerParams(collective_id=0, has_side_effects=True),
    )(
        defect, mass, block_diag, coupling,
        tile_rows.reshape(1, TD), tile_cols.reshape(1, TD),
    )


def solution(mesh):
    return jax.shard_map(
        on_device,
        mesh=mesh,
        in_specs=(
            P("blk", None),
            P("blk", None),
            P("blk", None, None),
            P("blk", None, None),
            P("blk"),
            P("blk"),
        ),
        out_specs=P("blk", None),
        check_vma=False,
    )
```

```python
import itertools

import jax
import jax.numpy as jnp
from jax import lax
from jax.experimental import pallas as pl
from jax.experimental.pallas import tpu as pltpu
from jax.sharding import PartitionSpec as P

N = 128
RB = 12
TD = 96
HALF = 48
B = 128
SHIFT = 1.5
F32 = jnp.float32
BF16 = jnp.bfloat16
MESH = pl.DeviceIdType.MESH


def distance(offset):
    return sum(min(step, 4 - step) for step in offset[:3]) + 0.5 * offset[3]


OFFSETS = sorted(
    (o for o in itertools.product(range(4), range(4), range(4), range(2)) if any(o)),
    key=distance,
    reverse=True,
)


def code(offset):
    return offset[0] * 32 + offset[1] * 8 + offset[2] * 2 + offset[3]


def opposite(offset):
    return tuple((4 - step) % 4 for step in offset[:3]) + (offset[3],)


FAR = 14
FAR_CODES = [code(o) for o in OFFSETS[:FAR]]


def dot(a, b):
    return lax.dot_general(a, b, (((1,), (0,)), ((), ())), preferred_element_type=F32)


def dot_nt(a, b):
    return lax.dot_general(a, b, (((1,), (1,)), ((), ())), preferred_element_type=F32)


def iota(shape, dim):
    return lax.broadcasted_iota(jnp.int32, shape, dim)


def halves(x):
    high = x.astype(BF16)
    low = (x - high.astype(F32)).astype(BF16)
    return high, low


def total(x):
    return jnp.sum(jnp.sum(x, axis=0, keepdims=True), axis=1, keepdims=True)


def divided_by_rb(x):
    return lax.shift_right_logical(x * 21846, 18)


def kernel(
    defect_hbm, mass_hbm, diag_hbm, coup_hbm, rows_hbm, cols_hbm, out_ref,
    indices, vectors, raw, raw_diag, weights, index_rows, perm_vmem, perm_smem,
    products, oh_fetch_out, oh_push_in, oh_cols, oh_push_out, oh_local,
    oh_fetch_in, req_out, req_in, xp_out, xp_in, x_far, f_out, f_in,
    load_sem, small_sem, perm_sem, send_sem, recv_sem,
):
    me = lax.axis_index("blk")
    y, z, x, c = me // 32, (me // 8) % 4, (me // 2) % 4, me % 2
    y_part = [((y + d) % 4) * 32 for d in range(4)]
    z_part = [((z + d) % 4) * 8 for d in range(4)]
    x_part = [((x + d) % 4) * 2 for d in range(4)]
    c_part = [(c + d) % 2 for d in range(2)]
    yz = [[y_part[a] + z_part[b] for b in range(4)] for a in range(4)]
    xc = [[x_part[a] + c_part[b] for b in range(2)] for a in range(4)]
    peers = [yz[o[0]][o[1]] + xc[o[2]][o[3]] for o in OFFSETS]

    small_loads = [
        pltpu.make_async_copy(rows_hbm, indices.at[0], small_sem.at[0]),
        pltpu.make_async_copy(cols_hbm, indices.at[1], small_sem.at[1]),
        pltpu.make_async_copy(defect_hbm, vectors.at[0, 0:RB], small_sem.at[2]),
        pltpu.make_async_copy(mass_hbm, vectors.at[1, 0:RB], small_sem.at[3]),
    ]
    loads = [
        pltpu.make_async_copy(
            coup_hbm.at[pl.ds(16 * i, 16)], raw.at[pl.ds(16 * i, 16)], load_sem.at[i]
        )
        for i in range(6)
    ]
    loads.append(pltpu.make_async_copy(diag_hbm, raw_diag, load_sem.at[6]))
    for load in small_loads + loads:
        load.start()

    nothing = jnp.zeros((1, B), F32)
    req_in[0:1] = nothing
    f_in[0:1] = nothing
    xp_in[...] = jnp.zeros_like(xp_in)
    x_far[...] = jnp.zeros_like(x_far)

    barrier = pltpu.get_barrier_semaphore()
    for peer in peers:
        pl.semaphore_signal(barrier, inc=1, device_id=(peer,), device_id_type=MESH)

    lane_row = iota((1, B), 1)
    lanes = iota((B, B), 1)
    subs = iota((B, B), 0)
    products[...] = jnp.zeros_like(products)
    for load in small_loads:
        load.wait()
    index_rows[...] = jnp.zeros_like(index_rows)
    index_rows[0:1, 0:TD] = indices[0]
    index_rows[1:2, 0:TD] = indices[1]
    rows = index_rows[0:1, :]
    cols = index_rows[1:2, :]
    row_owner = divided_by_rb(rows)
    col_owner = divided_by_rb(cols)

    def hop(d):
        return jnp.where(d == 3, 1, d)

    def relative(owner):
        dy = (lax.shift_right_logical(owner, 5) - y) & 3
        dz = (lax.shift_right_logical(owner, 3) - z) & 3
        dx = (lax.shift_right_logical(owner, 1) - x) & 3
        dc = (owner + c) & 1
        return dy * 32 + dz * 8 + dx * 2 + dc, hop(dy) + hop(dz) + hop(dx) >= 5

    row_local = rows - row_owner * RB
    col_local = cols - col_owner * RB
    valid = lane_row < TD
    push = valid & (row_owner != me)
    fetch = valid & (row_owner == me)
    destination, is_far = relative(jnp.where(push, row_owner, col_owner))
    sub8 = iota((16, B), 0)
    kinds = [push & is_far, push & ~is_far, fetch & ~is_far, fetch & is_far]
    members = jnp.zeros((16, B), F32)
    for at, kind in enumerate(kinds):
        members = jnp.where((sub8 == at) & kind, 1.0, members)
    counts = jnp.sum(members, axis=1, keepdims=True)
    ranks = dot(members.astype(BF16), jnp.where(subs < lanes, 1.0, 0.0).astype(BF16))
    starts = [0.0, counts[0:1], HALF * 1.0, counts[2:3] + HALF]
    position = jnp.full((1, B), 1000.0, F32)
    for at, kind in enumerate(kinds):
        position = jnp.where(kind, ranks[at : at + 1] + starts[at], position)
    position = position.astype(jnp.int32)
    order = jnp.where(position == subs, 1.0, 0.0).astype(BF16)

    def as_f(v):
        return v.astype(F32)

    wanted = jnp.where(fetch, as_f(col_local) + 1.0, 0.0)
    target = jnp.where(push, as_f(row_local) + 1.0, 0.0)
    table = jnp.zeros((B, B), F32)
    for at, value in enumerate(
        (wanted, target, as_f(destination), as_f(col_local), as_f(row_local), as_f(lane_row))
    ):
        table = jnp.where(subs == at, value, table)
    table = table.astype(BF16)
    by_lane = dot_nt(table, order)
    by_sub = dot_nt(order, table)
    dest_lane = by_lane[2:3].astype(jnp.int32)
    row_local_lane = by_lane[4:5].astype(jnp.int32)
    perm_vmem[...] = by_lane[5:6].astype(jnp.int32)
    to_smem = pltpu.make_async_copy(perm_vmem, perm_smem, perm_sem)
    to_smem.start()

    sends_to = jnp.where((dest_lane == subs) & (lanes < TD), 1.0, 0.0)
    push_out = jnp.where(lanes < HALF, sends_to, 0.0).astype(BF16)
    oh_push_out[:, 0:B] = push_out
    oh_push_out[:, B:] = push_out
    slot = lanes % 16
    dest_sub = by_sub[HALF:TD, 2:3].astype(jnp.int32)
    oh_fetch_in[:, 0:B] = jnp.where(dest_sub == lanes[0:HALF], 1.0, 0.0).astype(BF16)
    far_codes = jnp.full((1, B), -1, jnp.int32)
    for at, value in enumerate(FAR_CODES):
        far_codes = jnp.where(lane_row == at, value, far_codes)
    oh_fetch_in[:, B:] = jnp.where(dest_sub == far_codes, 1.0, 0.0).astype(BF16)
    col_local_sub = by_sub[0:HALF, 3:4].astype(jnp.int32)
    oh_cols[...] = jnp.where(col_local_sub == iota((HALF, 16), 1), 1.0, 0.0).astype(BF16)
    lanes16 = iota((16, B), 1)
    local_target = jnp.where(
        (lanes16 >= HALF) & (lanes16 < TD),
        row_local_lane,
        jnp.where((lanes16 >= TD) & (lanes16 < TD + RB), lanes16 - TD, -1),
    )
    local = jnp.where(local_target == sub8, 1.0, 0.0).astype(BF16)
    oh_local[:, 0:B] = local
    oh_local[:, B:] = local

    own_rows = iota((16, B), 0) < RB
    u0 = jnp.where(own_rows, -vectors[0], 0.0)
    mass = jnp.where(own_rows, vectors[1] - SHIFT, 0.0)
    beta_part = total(u0 * u0)
    message = dot(sends_to.astype(BF16), by_sub.astype(BF16))
    req_out[...] = jnp.where(lanes < 2, message, jnp.where(lanes == 2, beta_part, 0.0))

    pl.semaphore_wait(barrier, N - 1)

    def send_one(source, landing, at, k):
        offset = OFFSETS[k]
        pltpu.make_async_remote_copy(
            src_ref=source(code(offset)), dst_ref=landing(code(opposite(offset))),
            send_sem=send_sem.at[at], recv_sem=recv_sem.at[at],
            device_id=(peers[k],), device_id_type=MESH,
        ).start()

    def send(source, landing, at, first=0, last=N - 1):
        for k in range(first, last):
            send_one(source, landing, at, k)

    def received(ref, at):
        pltpu.make_async_copy(ref, ref, recv_sem.at[at]).wait()

    def sent(ref, at):
        pltpu.make_async_copy(ref, ref, send_sem.at[at]).wait()

    one_row = pl.ds(0, N - 1)
    far_rows = pl.ds(0, FAR)
    rest_rows = pl.ds(0, N - 1 - FAR)
    send(lambda p: req_out.at[p : p + 1], lambda m: req_in.at[m : m + 1], 0)

    for load in loads:
        load.wait()
    to_smem.wait()

    def put(pair, tile, at):
        high, low = halves(tile.T)
        weights[pair, 0:B, at * B : (at + 1) * B] = high
        weights[pair, B:, at * B : (at + 1) * B] = low

    def in_order(at):
        return raw[jnp.minimum(jnp.maximum(perm_smem[0, at], 0), TD - 1)]

    for pair in range(HALF):
        put(pair, in_order(2 * pair), 0)
        put(pair, in_order(2 * pair + 1), 1)
    for pair in range(RB // 2):
        put(HALF + pair, raw_diag[2 * pair], 0)
        put(HALF + pair, raw_diag[2 * pair + 1], 1)

    rows16 = iota((16, B), 0)

    def tile_products(high, low, first_pair, pairs, between=lambda: None):
        lhs = jnp.concatenate(
            [jnp.concatenate([high, high], axis=1), jnp.concatenate([low, low], axis=1)], axis=0
        )
        out = jnp.zeros((16, B), F32)
        for i in range(pairs):
            got = dot(lhs, weights[first_pair + i])
            between()
            got = got[0:16] + got[16:32]
            out = jnp.where(
                rows16 == 2 * i, got[:, 0:B], jnp.where(rows16 == 2 * i + 1, got[:, B:], out)
            )
        return out

    def block_products(picked, first_pair, between=lambda: None):
        return tile_products(picked[:, 0:B], picked[:, B:], first_pair, 8, between)

    def send_push(at):
        send(
            lambda p: xp_out.at[at, 2, p : p + 1], lambda m: xp_in.at[at, 2, m : m + 1], 4 + at
        )

    def send_x(at):
        planes = slice(0, 2) if at else slice(0, 1)
        send(
            lambda p: xp_out.at[at, planes, p : p + 1],
            lambda m: x_far.at[at, planes, FAR_CODES.index(m) : FAR_CODES.index(m) + 1],
            8 + at, 0, FAR,
        )
        left = iter(range(FAR, N - 1))

        def more(count):
            for k in itertools.islice(left, count):
                send_one(
                    lambda p: xp_out.at[at, planes, p : p + 1],
                    lambda m: xp_in.at[at, planes, m : m + 1], 1 + at, k,
                )

        return more

    def push(high, low, at, between=lambda: None):
        picked = dot(oh_cols[...], jnp.concatenate([high, low], axis=1)).astype(BF16)
        for b in range(3):
            products[16 * b : 16 * b + 16] = block_products(
                picked[16 * b : 16 * b + 16], 8 * b, between
            )
        p_high, p_low = halves(products[...])
        xp_out[at, 2] = dot(oh_push_out[...], jnp.concatenate([p_high, p_low], axis=0))

    def make_x(vector, high, low, dots_row, at):
        rest = (vector - high.astype(F32) - low.astype(F32)).astype(BF16)
        stacked = jnp.concatenate([high, low, rest], axis=0)
        xp_out[at, 0] = dot(oh_fetch_out[:, 0:HALF], stacked)
        if at:
            xp_out[at, 1] = jnp.broadcast_to(dots_row, (B, B))

    def finish(vector, high, low, at, reduced, images):
        planes = slice(0, 2) if at else slice(0, 1)
        products[TD : TD + 16] = tile_products(high, low, HALF, RB // 2)
        received(xp_in.at[at, planes, rest_rows], 1 + at)
        near = jnp.concatenate(halves(xp_in[at, 0]), axis=1)
        picked = dot(oh_fetch_in[0:32, 0:B], near).astype(BF16)
        for b in range(2):
            products[HALF + 16 * b : HALF + 16 * b + 16] = block_products(
                picked[16 * b : 16 * b + 16], 24 + 8 * b
            )
        received(x_far.at[at, planes, far_rows], 8 + at)
        far = jnp.concatenate(halves(x_far[at, 0]), axis=1)
        picked = dot(oh_fetch_in[32:48, 0:B], near) + dot(oh_fetch_in[32:48, B : B + 16], far)
        products[HALF + 32 : TD] = block_products(picked.astype(BF16), 40)
        p_high, p_low = halves(products[...])
        here = mass * vector + dot(oh_local[...], jnp.concatenate([p_high, p_low], axis=0))
        sums = reduced()
        norm = sums[-1]
        for term, image in zip(sums, images):
            norm = norm - term * term
            here = here - term * image
        norm = jnp.sqrt(norm)
        scale = 1.0 / norm
        here = here * scale
        received(xp_in.at[at, 2, one_row], 4 + at)
        p_high, p_low = halves(xp_in[at, 2])
        image = here + scale * dot(oh_push_in[...], jnp.concatenate([p_high, p_low], axis=0))
        return sums[:-1], norm, scale, image

    def packed(values):
        row = jnp.zeros((1, B), F32)
        for i, value in enumerate(values):
            row = jnp.where(lane_row == i, value, row)
        return row

    def unpacked(row, count):
        return [
            jnp.sum(jnp.where(lane_row == i, row, 0.0), axis=1, keepdims=True)
            for i in range(count)
        ]

    u_high, u_low = halves(u0)
    push(u_high, u_low, 0)
    send_push(0)
    received(req_in.at[one_row], 0)
    req = req_in[...]
    asked = req[:, 0:1].astype(jnp.int32) - 1
    oh_fetch_out[...] = jnp.where((asked == slot) & (lanes < 48), 1.0, 0.0).astype(BF16)
    make_x(u0, u_high, u_low, None, 0)
    send_x(0)(N)
    landing = req[:, 1:2].astype(jnp.int32) - 1
    into = jnp.where(landing == lanes, 1.0, 0.0).T[0:16].astype(BF16)
    oh_push_in[:, 0:B] = into
    oh_push_in[:, B:] = into
    beta_row = jnp.where(lane_row == 2, jnp.sum(req, axis=0, keepdims=True), 0.0)
    beta_square = jnp.sum(beta_row, axis=1, keepdims=True) + beta_part
    _, beta, scale, w0 = finish(u0, u_high, u_low, 0, lambda: [beta_square], [])
    v0 = u0 * scale

    def apply_with_dots(vector, others, images, at):
        row = packed([total(other * vector) for other in others] + [total(vector * vector)])
        high, low = halves(vector)
        make_x(vector, high, low, row, at)
        more = send_x(at)
        push(high, low, at, lambda: more(5))
        more(N)
        send_push(at)

        def reduced():
            sums = jnp.sum(xp_in[at, 1], axis=0, keepdims=True) + row
            sums = sums + jnp.sum(x_far[at, 1], axis=0, keepdims=True)
            return unpacked(sums, len(others) + 1)

        return finish(vector, high, low, at, reduced, images)

    (h00,), h10, scale, w1 = apply_with_dots(w0, [v0], [w0], 1)
    v1 = (w0 - h00 * v0) * scale
    (h01, h11), h21, scale, w2 = apply_with_dots(w1, [v0, v1], [w0, w1], 2)
    v2 = (w1 - h01 * v0 - h11 * v1) * scale

    row = packed([total(v0 * w2), total(v1 * w2), total(v2 * w2), total(w2 * w2)])
    f_out[...] = jnp.broadcast_to(row, (8, B))
    send(lambda p: f_out.at[0:1], lambda m: f_in.at[m : m + 1], 7)
    received(f_in.at[one_row], 7)
    sums = jnp.sum(f_in[...], axis=0, keepdims=True) + row
    h02, h12, h22, square = unpacked(sums, 4)
    h32 = jnp.sqrt(square - h02 * h02 - h12 * h12 - h22 * h22)

    h00, h11, h22 = h00 + SHIFT, h11 + SHIFT, h22 + SHIFT
    g00 = h00 * h00 + h10 * h10
    g10 = h01 * h00 + h11 * h10
    g20 = h02 * h00 + h12 * h10
    g11 = h01 * h01 + h11 * h11 + h21 * h21
    g21 = h02 * h01 + h12 * h11 + h22 * h21
    g22 = h02 * h02 + h12 * h12 + h22 * h22 + h32 * h32
    l00 = jnp.sqrt(g00)
    l10, l20 = g10 / l00, g20 / l00
    l11 = jnp.sqrt(g11 - l10 * l10)
    l21 = (g21 - l20 * l10) / l11
    l22 = jnp.sqrt(g22 - l20 * l20 - l21 * l21)
    t0 = beta * h00 / l00
    t1 = (beta * h01 - l10 * t0) / l11
    t2 = (beta * h02 - l20 * t0 - l21 * t1) / l22
    m2 = t2 / l22
    m1 = (t1 - l21 * m2) / l11
    m0 = (t0 - l10 * m1 - l20 * m2) / l00
    update = m0 * v0 + m1 * v1 + m2 * v2
    out_ref[...] = update[0:RB]

    sent(req_out.at[one_row], 0)
    for at in range(3):
        planes = slice(0, 2) if at else slice(0, 1)
        sent(xp_in.at[at, planes, rest_rows], 1 + at)
        sent(x_far.at[at, planes, far_rows], 8 + at)
        sent(xp_in.at[at, 2, one_row], 4 + at)
    sent(f_in.at[one_row], 7)


def on_device(defect, mass, block_diag, coupling, tile_rows, tile_cols):
    vmem = pl.BlockSpec(memory_space=pltpu.VMEM)
    hbm = pl.BlockSpec(memory_space=pl.ANY)
    return pl.pallas_call(
        kernel,
        out_shape=pltpu.VMEM(defect.shape, F32),
        in_specs=[hbm] * 6,
        out_specs=vmem,
        scratch_shapes=[
            pltpu.VMEM((2, 1, TD), jnp.int32),
            pltpu.VMEM((2, 16, B), F32),
            pltpu.VMEM((TD, B, B), F32),
            pltpu.VMEM((RB, B, B), F32),
            pltpu.VMEM((54, 2 * B, 2 * B), BF16),
            pltpu.VMEM((8, B), jnp.int32),
            pltpu.VMEM((1, B), jnp.int32),
            pltpu.SMEM((1, B), jnp.int32),
            pltpu.VMEM((B, B), F32),
            pltpu.VMEM((B, B), BF16),
            pltpu.VMEM((16, 2 * B), BF16),
            pltpu.VMEM((HALF, 16), BF16),
            pltpu.VMEM((B, 2 * B), BF16),
            pltpu.VMEM((16, 2 * B), BF16),
            pltpu.VMEM((HALF, 2 * B), BF16),
            pltpu.VMEM((N, B), F32),
            pltpu.VMEM((N, B), F32),
            pltpu.VMEM((3, 3, N, B), F32),
            pltpu.VMEM((3, 3, N, B), F32),
            pltpu.VMEM((3, 2, 16, B), F32),
            pltpu.VMEM((8, B), F32),
            pltpu.VMEM((N, B), F32),
            pltpu.SemaphoreType.DMA((7,)),
            pltpu.SemaphoreType.DMA((4,)),
            pltpu.SemaphoreType.DMA,
            pltpu.SemaphoreType.DMA((11,)),
            pltpu.SemaphoreType.DMA((11,)),
        ],
        compiler_params=pltpu.CompilerParams(collective_id=0, has_side_effects=True),
    )(
        defect, mass, block_diag, coupling,
        tile_rows.reshape(1, TD), tile_cols.reshape(1, TD),
    )


def solution(mesh):
    return jax.shard_map(
        on_device,
        mesh=mesh,
        in_specs=(
            P("blk", None),
            P("blk", None),
            P("blk", None, None),
            P("blk", None, None),
            P("blk"),
            P("blk"),
        ),
        out_specs=P("blk", None),
        check_vma=False,
    )
```

```python
import itertools

import jax
import jax.numpy as jnp
from jax import lax
from jax.experimental import pallas as pl
from jax.experimental.pallas import tpu as pltpu
from jax.sharding import PartitionSpec as P

N = 128
RB = 12
TD = 96
HALF = 48
B = 128
SHIFT = 1.5
F32 = jnp.float32
BF16 = jnp.bfloat16
MESH = pl.DeviceIdType.MESH


def distance(offset):
    return sum(min(step, 4 - step) for step in offset[:3])


def mixed(offset):
    at = offset[0] * 32 + offset[1] * 8 + offset[2] * 2 + offset[3]
    return at * 37 % 128


OFFSETS = sorted(
    (o for o in itertools.product(range(4), range(4), range(4), range(2)) if any(o)),
    key=lambda o: (-distance(o), mixed(o)),
)


def code(offset):
    return offset[0] * 32 + offset[1] * 8 + offset[2] * 2 + offset[3]


def opposite(offset):
    return tuple((4 - step) % 4 for step in offset[:3]) + (offset[3],)


FAR = 14
FAR_CODES = [code(o) for o in OFFSETS[:FAR]]


def dot(a, b):
    return lax.dot_general(a, b, (((1,), (0,)), ((), ())), preferred_element_type=F32)


def dot_nt(a, b):
    return lax.dot_general(a, b, (((1,), (1,)), ((), ())), preferred_element_type=F32)


def iota(shape, dim):
    return lax.broadcasted_iota(jnp.int32, shape, dim)


def halves(x):
    high = x.astype(BF16)
    low = (x - high.astype(F32)).astype(BF16)
    return high, low


def total(x):
    return jnp.sum(jnp.sum(x, axis=0, keepdims=True), axis=1, keepdims=True)


def divided_by_rb(x):
    return lax.shift_right_logical(x * 21846, 18)


def kernel(
    defect_hbm, mass_hbm, diag_hbm, coup_hbm, rows_hbm, cols_hbm, out_ref,
    indices, vectors, raw, raw_diag, weights, index_rows, perm_vmem, perm_smem,
    products, oh_fetch_out, oh_push_in, oh_cols, oh_push_out, oh_local,
    oh_fetch_in, req_out, req_in, xp_out, xp_in, x_far, f_out, f_in,
    load_sem, small_sem, perm_sem, send_sem, recv_sem,
):
    me = lax.axis_index("blk")
    y, z, x, c = me // 32, (me // 8) % 4, (me // 2) % 4, me % 2
    y_part = [((y + d) % 4) * 32 for d in range(4)]
    z_part = [((z + d) % 4) * 8 for d in range(4)]
    x_part = [((x + d) % 4) * 2 for d in range(4)]
    c_part = [(c + d) % 2 for d in range(2)]
    yz = [[y_part[a] + z_part[b] for b in range(4)] for a in range(4)]
    xc = [[x_part[a] + c_part[b] for b in range(2)] for a in range(4)]
    peers = [yz[o[0]][o[1]] + xc[o[2]][o[3]] for o in OFFSETS]

    small_loads = [
        pltpu.make_async_copy(rows_hbm, indices.at[0], small_sem.at[0]),
        pltpu.make_async_copy(cols_hbm, indices.at[1], small_sem.at[1]),
        pltpu.make_async_copy(defect_hbm, vectors.at[0, 0:RB], small_sem.at[2]),
        pltpu.make_async_copy(mass_hbm, vectors.at[1, 0:RB], small_sem.at[3]),
    ]
    loads = [
        pltpu.make_async_copy(
            coup_hbm.at[pl.ds(16 * i, 16)], raw.at[pl.ds(16 * i, 16)], load_sem.at[i]
        )
        for i in range(6)
    ]
    loads.append(pltpu.make_async_copy(diag_hbm, raw_diag, load_sem.at[6]))
    for load in small_loads + loads:
        load.start()

    nothing = jnp.zeros((1, B), F32)
    req_in[0:1] = nothing
    f_in[0:1] = nothing
    xp_in[...] = jnp.zeros_like(xp_in)
    x_far[...] = jnp.zeros_like(x_far)

    barrier = pltpu.get_barrier_semaphore()
    for peer in peers:
        pl.semaphore_signal(barrier, inc=1, device_id=(peer,), device_id_type=MESH)

    lane_row = iota((1, B), 1)
    lanes = iota((B, B), 1)
    subs = iota((B, B), 0)
    products[...] = jnp.zeros_like(products)
    for load in small_loads:
        load.wait()
    index_rows[...] = jnp.zeros_like(index_rows)
    index_rows[0:1, 0:TD] = indices[0]
    index_rows[1:2, 0:TD] = indices[1]
    rows = index_rows[0:1, :]
    cols = index_rows[1:2, :]
    row_owner = divided_by_rb(rows)
    col_owner = divided_by_rb(cols)

    def hop(d):
        return jnp.where(d == 3, 1, d)

    def relative(owner):
        dy = (lax.shift_right_logical(owner, 5) - y) & 3
        dz = (lax.shift_right_logical(owner, 3) - z) & 3
        dx = (lax.shift_right_logical(owner, 1) - x) & 3
        dc = (owner + c) & 1
        return dy * 32 + dz * 8 + dx * 2 + dc, hop(dy) + hop(dz) + hop(dx) >= 5

    row_local = rows - row_owner * RB
    col_local = cols - col_owner * RB
    valid = lane_row < TD
    push = valid & (row_owner != me)
    fetch = valid & (row_owner == me)
    destination, is_far = relative(jnp.where(push, row_owner, col_owner))
    sub8 = iota((16, B), 0)
    kinds = [push & is_far, push & ~is_far, fetch & ~is_far, fetch & is_far]
    members = jnp.zeros((16, B), F32)
    for at, kind in enumerate(kinds):
        members = jnp.where((sub8 == at) & kind, 1.0, members)
    counts = jnp.sum(members, axis=1, keepdims=True)
    ranks = dot(members.astype(BF16), jnp.where(subs < lanes, 1.0, 0.0).astype(BF16))
    starts = [0.0, counts[0:1], HALF * 1.0, counts[2:3] + HALF]
    position = jnp.full((1, B), 1000.0, F32)
    for at, kind in enumerate(kinds):
        position = jnp.where(kind, ranks[at : at + 1] + starts[at], position)
    position = position.astype(jnp.int32)
    order = jnp.where(position == subs, 1.0, 0.0).astype(BF16)

    def as_f(v):
        return v.astype(F32)

    wanted = jnp.where(fetch, as_f(col_local) + 1.0, 0.0)
    target = jnp.where(push, as_f(row_local) + 1.0, 0.0)
    table = jnp.zeros((B, B), F32)
    for at, value in enumerate(
        (wanted, target, as_f(destination), as_f(col_local), as_f(row_local), as_f(lane_row))
    ):
        table = jnp.where(subs == at, value, table)
    table = table.astype(BF16)
    by_lane = dot_nt(table, order)
    by_sub = dot_nt(order, table)
    dest_lane = by_lane[2:3].astype(jnp.int32)
    row_local_lane = by_lane[4:5].astype(jnp.int32)
    perm_vmem[...] = by_lane[5:6].astype(jnp.int32)
    to_smem = pltpu.make_async_copy(perm_vmem, perm_smem, perm_sem)
    to_smem.start()

    sends_to = jnp.where((dest_lane == subs) & (lanes < TD), 1.0, 0.0)
    push_out = jnp.where(lanes < HALF, sends_to, 0.0).astype(BF16)
    oh_push_out[:, 0:B] = push_out
    oh_push_out[:, B:] = push_out
    slot = lanes % 16
    dest_sub = by_sub[HALF:TD, 2:3].astype(jnp.int32)
    oh_fetch_in[:, 0:B] = jnp.where(dest_sub == lanes[0:HALF], 1.0, 0.0).astype(BF16)
    far_codes = jnp.full((1, B), -1, jnp.int32)
    for at, value in enumerate(FAR_CODES):
        far_codes = jnp.where(lane_row == at, value, far_codes)
    oh_fetch_in[:, B:] = jnp.where(dest_sub == far_codes, 1.0, 0.0).astype(BF16)
    col_local_sub = by_sub[0:HALF, 3:4].astype(jnp.int32)
    oh_cols[...] = jnp.where(col_local_sub == iota((HALF, 16), 1), 1.0, 0.0).astype(BF16)
    lanes16 = iota((16, B), 1)
    local_target = jnp.where(
        (lanes16 >= HALF) & (lanes16 < TD),
        row_local_lane,
        jnp.where((lanes16 >= TD) & (lanes16 < TD + RB), lanes16 - TD, -1),
    )
    local = jnp.where(local_target == sub8, 1.0, 0.0).astype(BF16)
    oh_local[:, 0:B] = local
    oh_local[:, B:] = local

    own_rows = iota((16, B), 0) < RB
    u0 = jnp.where(own_rows, -vectors[0], 0.0)
    mass = jnp.where(own_rows, vectors[1] - SHIFT, 0.0)
    beta_part = total(u0 * u0)
    message = dot(sends_to.astype(BF16), by_sub.astype(BF16))
    req_out[...] = jnp.where(lanes < 2, message, jnp.where(lanes == 2, beta_part, 0.0))

    pl.semaphore_wait(barrier, N - 1)

    def send_one(source, landing, at, k):
        offset = OFFSETS[k]
        pltpu.make_async_remote_copy(
            src_ref=source(code(offset)), dst_ref=landing(code(opposite(offset))),
            send_sem=send_sem.at[at], recv_sem=recv_sem.at[at],
            device_id=(peers[k],), device_id_type=MESH,
        ).start()

    def send(source, landing, at, first=0, last=N - 1):
        for k in range(first, last):
            send_one(source, landing, at, k)

    def received(ref, at):
        pltpu.make_async_copy(ref, ref, recv_sem.at[at]).wait()

    def sent(ref, at):
        pltpu.make_async_copy(ref, ref, send_sem.at[at]).wait()

    one_row = pl.ds(0, N - 1)
    far_rows = pl.ds(0, FAR)
    rest_rows = pl.ds(0, N - 1 - FAR)
    send(lambda p: req_out.at[p : p + 1], lambda m: req_in.at[m : m + 1], 0)

    for load in loads:
        load.wait()
    to_smem.wait()

    def put(pair, tile, at):
        high, low = halves(tile.T)
        weights[pair, 0:B, at * B : (at + 1) * B] = high
        weights[pair, B:, at * B : (at + 1) * B] = low

    def in_order(at):
        return raw[jnp.minimum(jnp.maximum(perm_smem[0, at], 0), TD - 1)]

    for pair in range(HALF):
        put(pair, in_order(2 * pair), 0)
        put(pair, in_order(2 * pair + 1), 1)
    for pair in range(RB // 2):
        put(HALF + pair, raw_diag[2 * pair], 0)
        put(HALF + pair, raw_diag[2 * pair + 1], 1)

    rows16 = iota((16, B), 0)

    def tile_products(high, low, first_pair, pairs, between=lambda: None):
        lhs = jnp.concatenate(
            [jnp.concatenate([high, high], axis=1), jnp.concatenate([low, low], axis=1)], axis=0
        )
        out = jnp.zeros((16, B), F32)
        for i in range(pairs):
            got = dot(lhs, weights[first_pair + i])
            between()
            got = got[0:16] + got[16:32]
            out = jnp.where(
                rows16 == 2 * i, got[:, 0:B], jnp.where(rows16 == 2 * i + 1, got[:, B:], out)
            )
        return out

    def block_products(picked, first_pair, between=lambda: None):
        return tile_products(picked[:, 0:B], picked[:, B:], first_pair, 8, between)

    def send_push(at):
        send(
            lambda p: xp_out.at[at, 2, p : p + 1], lambda m: xp_in.at[at, 2, m : m + 1], 4 + at
        )

    def send_x(at):
        planes = slice(0, 2) if at else slice(0, 1)
        send(
            lambda p: xp_out.at[at, planes, p : p + 1],
            lambda m: x_far.at[at, planes, FAR_CODES.index(m) : FAR_CODES.index(m) + 1],
            8 + at, 0, FAR,
        )
        left = iter(range(FAR, N - 1))

        def more(count):
            for k in itertools.islice(left, count):
                send_one(
                    lambda p: xp_out.at[at, planes, p : p + 1],
                    lambda m: xp_in.at[at, planes, m : m + 1], 1 + at, k,
                )

        return more

    def push(high, low, at, between=lambda: None):
        picked = dot(oh_cols[...], jnp.concatenate([high, low], axis=1)).astype(BF16)
        for b in range(3):
            products[16 * b : 16 * b + 16] = block_products(
                picked[16 * b : 16 * b + 16], 8 * b, between
            )
        p_high, p_low = halves(products[...])
        xp_out[at, 2] = dot(oh_push_out[...], jnp.concatenate([p_high, p_low], axis=0))

    def make_x(vector, high, low, dots_row, at):
        rest = (vector - high.astype(F32) - low.astype(F32)).astype(BF16)
        stacked = jnp.concatenate([high, low, rest], axis=0)
        xp_out[at, 0] = dot(oh_fetch_out[:, 0:HALF], stacked)
        if at:
            xp_out[at, 1] = jnp.broadcast_to(dots_row, (B, B))

    def finish(vector, high, low, at, reduced, images):
        planes = slice(0, 2) if at else slice(0, 1)
        products[TD : TD + 16] = tile_products(high, low, HALF, RB // 2)
        received(xp_in.at[at, planes, rest_rows], 1 + at)
        near = jnp.concatenate(halves(xp_in[at, 0]), axis=1)
        picked = dot(oh_fetch_in[0:32, 0:B], near).astype(BF16)
        for b in range(2):
            products[HALF + 16 * b : HALF + 16 * b + 16] = block_products(
                picked[16 * b : 16 * b + 16], 24 + 8 * b
            )
        received(x_far.at[at, planes, far_rows], 8 + at)
        far = jnp.concatenate(halves(x_far[at, 0]), axis=1)
        picked = dot(oh_fetch_in[32:48, 0:B], near) + dot(oh_fetch_in[32:48, B : B + 16], far)
        products[HALF + 32 : TD] = block_products(picked.astype(BF16), 40)
        p_high, p_low = halves(products[...])
        here = mass * vector + dot(oh_local[...], jnp.concatenate([p_high, p_low], axis=0))
        sums = reduced()
        norm = sums[-1]
        for term, image in zip(sums, images):
            norm = norm - term * term
            here = here - term * image
        norm = jnp.sqrt(norm)
        scale = 1.0 / norm
        here = here * scale
        received(xp_in.at[at, 2, one_row], 4 + at)
        p_high, p_low = halves(xp_in[at, 2])
        image = here + scale * dot(oh_push_in[...], jnp.concatenate([p_high, p_low], axis=0))
        return sums[:-1], norm, scale, image

    def packed(values):
        row = jnp.zeros((1, B), F32)
        for i, value in enumerate(values):
            row = jnp.where(lane_row == i, value, row)
        return row

    def unpacked(row, count):
        return [
            jnp.sum(jnp.where(lane_row == i, row, 0.0), axis=1, keepdims=True)
            for i in range(count)
        ]

    u_high, u_low = halves(u0)
    push(u_high, u_low, 0)
    received(req_in.at[one_row], 0)
    req = req_in[...]
    asked = req[:, 0:1].astype(jnp.int32) - 1
    oh_fetch_out[...] = jnp.where((asked == slot) & (lanes < 48), 1.0, 0.0).astype(BF16)
    make_x(u0, u_high, u_low, None, 0)
    send_x(0)(N)
    send_push(0)
    landing = req[:, 1:2].astype(jnp.int32) - 1
    into = jnp.where(landing == lanes, 1.0, 0.0).T[0:16].astype(BF16)
    oh_push_in[:, 0:B] = into
    oh_push_in[:, B:] = into
    beta_row = jnp.where(lane_row == 2, jnp.sum(req, axis=0, keepdims=True), 0.0)
    beta_square = jnp.sum(beta_row, axis=1, keepdims=True) + beta_part
    _, beta, scale, w0 = finish(u0, u_high, u_low, 0, lambda: [beta_square], [])
    v0 = u0 * scale

    def apply_with_dots(vector, others, images, at):
        row = packed([total(other * vector) for other in others] + [total(vector * vector)])
        high, low = halves(vector)
        make_x(vector, high, low, row, at)
        more = send_x(at)
        push(high, low, at, lambda: more(6))
        more(N)
        send_push(at)

        def reduced():
            sums = jnp.sum(xp_in[at, 1], axis=0, keepdims=True) + row
            sums = sums + jnp.sum(x_far[at, 1], axis=0, keepdims=True)
            return unpacked(sums, len(others) + 1)

        return finish(vector, high, low, at, reduced, images)

    (h00,), h10, scale, w1 = apply_with_dots(w0, [v0], [w0], 1)
    v1 = (w0 - h00 * v0) * scale
    (h01, h11), h21, scale, w2 = apply_with_dots(w1, [v0, v1], [w0, w1], 2)
    v2 = (w1 - h01 * v0 - h11 * v1) * scale

    row = packed([total(v0 * w2), total(v1 * w2), total(v2 * w2), total(w2 * w2)])
    f_out[...] = jnp.broadcast_to(row, (8, B))
    send(lambda p: f_out.at[0:1], lambda m: f_in.at[m : m + 1], 7)
    h00, h11 = h00 + SHIFT, h11 + SHIFT
    l00_inv = 1.0 / jnp.sqrt(h00 * h00 + h10 * h10)
    l10 = (h01 * h00 + h11 * h10) * l00_inv
    l11_inv = 1.0 / jnp.sqrt(h01 * h01 + h11 * h11 + h21 * h21 - l10 * l10)
    t0 = beta * h00 * l00_inv
    t1 = (beta * h01 - l10 * t0) * l11_inv

    sent(req_out.at[one_row], 0)
    for at in range(3):
        planes = slice(0, 2) if at else slice(0, 1)
        sent(xp_in.at[at, planes, rest_rows], 1 + at)
        sent(x_far.at[at, planes, far_rows], 8 + at)
        sent(xp_in.at[at, 2, one_row], 4 + at)
    received(f_in.at[one_row], 7)
    sums = jnp.sum(f_in[...], axis=0, keepdims=True) + row
    h02, h12, h22, square = unpacked(sums, 4)
    h32_square = square - h02 * h02 - h12 * h12 - h22 * h22
    h22 = h22 + SHIFT
    l20 = (h02 * h00 + h12 * h10) * l00_inv
    l21 = (h02 * h01 + h12 * h11 + h22 * h21 - l20 * l10) * l11_inv
    pivot = h02 * h02 + h12 * h12 + h22 * h22 + h32_square - l20 * l20 - l21 * l21
    m2 = (beta * h02 - l20 * t0 - l21 * t1) / pivot
    m1 = (t1 - l21 * m2) * l11_inv
    m0 = (t0 - l10 * m1 - l20 * m2) * l00_inv
    update = m0 * v0 + m1 * v1 + m2 * v2
    out_ref[...] = update[0:RB]

    sent(f_in.at[one_row], 7)


def on_device(defect, mass, block_diag, coupling, tile_rows, tile_cols):
    vmem = pl.BlockSpec(memory_space=pltpu.VMEM)
    hbm = pl.BlockSpec(memory_space=pl.ANY)
    return pl.pallas_call(
        kernel,
        out_shape=pltpu.VMEM(defect.shape, F32),
        in_specs=[hbm] * 6,
        out_specs=vmem,
        scratch_shapes=[
            pltpu.VMEM((2, 1, TD), jnp.int32),
            pltpu.VMEM((2, 16, B), F32),
            pltpu.VMEM((TD, B, B), F32),
            pltpu.VMEM((RB, B, B), F32),
            pltpu.VMEM((54, 2 * B, 2 * B), BF16),
            pltpu.VMEM((8, B), jnp.int32),
            pltpu.VMEM((1, B), jnp.int32),
            pltpu.SMEM((1, B), jnp.int32),
            pltpu.VMEM((B, B), F32),
            pltpu.VMEM((B, B), BF16),
            pltpu.VMEM((16, 2 * B), BF16),
            pltpu.VMEM((HALF, 16), BF16),
            pltpu.VMEM((B, 2 * B), BF16),
            pltpu.VMEM((16, 2 * B), BF16),
            pltpu.VMEM((HALF, 2 * B), BF16),
            pltpu.VMEM((N, B), F32),
            pltpu.VMEM((N, B), F32),
            pltpu.VMEM((3, 3, N, B), F32),
            pltpu.VMEM((3, 3, N, B), F32),
            pltpu.VMEM((3, 2, 16, B), F32),
            pltpu.VMEM((8, B), F32),
            pltpu.VMEM((N, B), F32),
            pltpu.SemaphoreType.DMA((7,)),
            pltpu.SemaphoreType.DMA((4,)),
            pltpu.SemaphoreType.DMA,
            pltpu.SemaphoreType.DMA((11,)),
            pltpu.SemaphoreType.DMA((11,)),
        ],
        compiler_params=pltpu.CompilerParams(collective_id=0, has_side_effects=True),
    )(
        defect, mass, block_diag, coupling,
        tile_rows.reshape(1, TD), tile_cols.reshape(1, TD),
    )


def solution(mesh):
    return jax.shard_map(
        on_device,
        mesh=mesh,
        in_specs=(
            P("blk", None),
            P("blk", None),
            P("blk", None, None),
            P("blk", None, None),
            P("blk"),
            P("blk"),
        ),
        out_specs=P("blk", None),
        check_vma=False,
    )
```

```python
import itertools

import jax
import jax.numpy as jnp
from jax import lax
from jax.experimental import pallas as pl
from jax.experimental.pallas import tpu as pltpu
from jax.sharding import PartitionSpec as P

N = 128
RB = 12
TD = 96
HALF = 48
B = 128
SHIFT = 1.5
F32 = jnp.float32
BF16 = jnp.bfloat16
MESH = pl.DeviceIdType.MESH


def distance(offset):
    return sum(min(step, 4 - step) for step in offset[:3])


def mixed(offset):
    at = offset[0] * 32 + offset[1] * 8 + offset[2] * 2 + offset[3]
    return at * 37 % 128


OFFSETS = sorted(
    (o for o in itertools.product(range(4), range(4), range(4), range(2)) if any(o)),
    key=lambda o: (-distance(o), mixed(o)),
)


def code(offset):
    return offset[0] * 32 + offset[1] * 8 + offset[2] * 2 + offset[3]


def opposite(offset):
    return tuple((4 - step) % 4 for step in offset[:3]) + (offset[3],)


FAR = 14
FAR_CODES = [code(o) for o in OFFSETS[:FAR]]


def dot(a, b):
    return lax.dot_general(a, b, (((1,), (0,)), ((), ())), preferred_element_type=F32)


def dot_nt(a, b):
    return lax.dot_general(a, b, (((1,), (1,)), ((), ())), preferred_element_type=F32)


def iota(shape, dim):
    return lax.broadcasted_iota(jnp.int32, shape, dim)


def halves(x):
    high = x.astype(BF16)
    low = (x - high.astype(F32)).astype(BF16)
    return high, low


def total(x):
    return jnp.sum(jnp.sum(x, axis=0, keepdims=True), axis=1, keepdims=True)


def divided_by_rb(x):
    return lax.shift_right_logical(x * 21846, 18)


def kernel(
    defect_hbm, mass_hbm, diag_hbm, coup_hbm, rows_hbm, cols_hbm, out_ref,
    indices, vectors, raw, raw_diag, weights, index_rows, perm_vmem, perm_smem,
    products, oh_fetch_out, oh_push_in, oh_cols, oh_push_out, oh_local,
    oh_fetch_in, req_out, req_in, xp_out, xp_in, x_far, f_out, f_in,
    load_sem, small_sem, perm_sem, send_sem, recv_sem,
):
    me = lax.axis_index("blk")
    y, z, x, c = me // 32, (me // 8) % 4, (me // 2) % 4, me % 2
    y_part = [((y + d) % 4) * 32 for d in range(4)]
    z_part = [((z + d) % 4) * 8 for d in range(4)]
    x_part = [((x + d) % 4) * 2 for d in range(4)]
    c_part = [(c + d) % 2 for d in range(2)]
    yz = [[y_part[a] + z_part[b] for b in range(4)] for a in range(4)]
    xc = [[x_part[a] + c_part[b] for b in range(2)] for a in range(4)]
    peers = [yz[o[0]][o[1]] + xc[o[2]][o[3]] for o in OFFSETS]

    small_loads = [
        pltpu.make_async_copy(rows_hbm, indices.at[0], small_sem.at[0]),
        pltpu.make_async_copy(cols_hbm, indices.at[1], small_sem.at[1]),
        pltpu.make_async_copy(defect_hbm, vectors.at[0, 0:RB], small_sem.at[2]),
        pltpu.make_async_copy(mass_hbm, vectors.at[1, 0:RB], small_sem.at[3]),
    ]
    loads = [
        pltpu.make_async_copy(
            coup_hbm.at[pl.ds(16 * i, 16)], raw.at[pl.ds(16 * i, 16)], load_sem.at[i]
        )
        for i in range(6)
    ]
    loads.append(pltpu.make_async_copy(diag_hbm, raw_diag, load_sem.at[6]))
    for load in small_loads + loads:
        load.start()

    nothing = jnp.zeros((1, B), F32)
    req_in[0:1] = nothing
    f_in[0:1] = nothing
    xp_in[...] = jnp.zeros_like(xp_in)
    x_far[...] = jnp.zeros_like(x_far)

    barrier = pltpu.get_barrier_semaphore()
    for peer in peers:
        pl.semaphore_signal(barrier, inc=1, device_id=(peer,), device_id_type=MESH)

    lane_row = iota((1, B), 1)
    lanes = iota((B, B), 1)
    subs = iota((B, B), 0)
    products[...] = jnp.zeros_like(products)
    for load in small_loads:
        load.wait()
    index_rows[...] = jnp.zeros_like(index_rows)
    index_rows[0:1, 0:TD] = indices[0]
    index_rows[1:2, 0:TD] = indices[1]
    rows = index_rows[0:1, :]
    cols = index_rows[1:2, :]
    row_owner = divided_by_rb(rows)
    col_owner = divided_by_rb(cols)

    def hop(d):
        return jnp.where(d == 3, 1, d)

    def relative(owner):
        dy = (lax.shift_right_logical(owner, 5) - y) & 3
        dz = (lax.shift_right_logical(owner, 3) - z) & 3
        dx = (lax.shift_right_logical(owner, 1) - x) & 3
        dc = (owner + c) & 1
        return dy * 32 + dz * 8 + dx * 2 + dc, hop(dy) + hop(dz) + hop(dx) >= 5

    row_local = rows - row_owner * RB
    col_local = cols - col_owner * RB
    valid = lane_row < TD
    push = valid & (row_owner != me)
    fetch = valid & (row_owner == me)
    destination, is_far = relative(jnp.where(push, row_owner, col_owner))
    sub8 = iota((16, B), 0)
    kinds = [push & is_far, push & ~is_far, fetch & ~is_far, fetch & is_far]
    members = jnp.zeros((16, B), F32)
    for at, kind in enumerate(kinds):
        members = jnp.where((sub8 == at) & kind, 1.0, members)
    counts = jnp.sum(members, axis=1, keepdims=True)
    ranks = dot(members.astype(BF16), jnp.where(subs < lanes, 1.0, 0.0).astype(BF16))
    starts = [0.0, counts[0:1], HALF * 1.0, counts[2:3] + HALF]
    position = jnp.full((1, B), 1000.0, F32)
    for at, kind in enumerate(kinds):
        position = jnp.where(kind, ranks[at : at + 1] + starts[at], position)
    position = position.astype(jnp.int32)
    order = jnp.where(position == subs, 1.0, 0.0).astype(BF16)

    def as_f(v):
        return v.astype(F32)

    wanted = jnp.where(fetch, as_f(col_local) + 1.0, 0.0)
    target = jnp.where(push, as_f(row_local) + 1.0, 0.0)
    table = jnp.zeros((B, B), F32)
    for at, value in enumerate(
        (wanted, target, as_f(destination), as_f(col_local), as_f(row_local), as_f(lane_row))
    ):
        table = jnp.where(subs == at, value, table)
    table = table.astype(BF16)
    by_lane = dot_nt(table, order)
    by_sub = dot_nt(order, table)
    dest_lane = by_lane[2:3].astype(jnp.int32)
    row_local_lane = by_lane[4:5].astype(jnp.int32)
    perm_vmem[...] = by_lane[5:6].astype(jnp.int32)
    to_smem = pltpu.make_async_copy(perm_vmem, perm_smem, perm_sem)
    to_smem.start()

    sends_to = jnp.where((dest_lane == subs) & (lanes < TD), 1.0, 0.0)
    push_out = jnp.where(lanes < HALF, sends_to, 0.0).astype(BF16)
    oh_push_out[:, 0:B] = push_out
    oh_push_out[:, B:] = push_out
    slot = lanes % 16
    dest_sub = by_sub[HALF:TD, 2:3].astype(jnp.int32)
    oh_fetch_in[:, 0:B] = jnp.where(dest_sub == lanes[0:HALF], 1.0, 0.0).astype(BF16)
    far_codes = jnp.full((1, B), -1, jnp.int32)
    for at, value in enumerate(FAR_CODES):
        far_codes = jnp.where(lane_row == at, value, far_codes)
    oh_fetch_in[:, B:] = jnp.where(dest_sub == far_codes, 1.0, 0.0).astype(BF16)
    col_local_sub = by_sub[0:HALF, 3:4].astype(jnp.int32)
    oh_cols[...] = jnp.where(col_local_sub == iota((HALF, 16), 1), 1.0, 0.0).astype(BF16)
    lanes16 = iota((16, B), 1)
    local_target = jnp.where(
        (lanes16 >= HALF) & (lanes16 < TD),
        row_local_lane,
        jnp.where((lanes16 >= TD) & (lanes16 < TD + RB), lanes16 - TD, -1),
    )
    local = jnp.where(local_target == sub8, 1.0, 0.0).astype(BF16)
    oh_local[:, 0:B] = local
    oh_local[:, B:] = local

    own_rows = iota((16, B), 0) < RB
    u0 = jnp.where(own_rows, -vectors[0], 0.0)
    mass = jnp.where(own_rows, vectors[1] - SHIFT, 0.0)
    beta_part = total(u0 * u0)
    message = dot(sends_to.astype(BF16), by_sub.astype(BF16))
    req_out[...] = jnp.where(lanes < 2, message, jnp.where(lanes == 2, beta_part, 0.0))

    pl.semaphore_wait(barrier, N - 1)

    def send_one(source, landing, at, k):
        offset = OFFSETS[k]
        pltpu.make_async_remote_copy(
            src_ref=source(code(offset)), dst_ref=landing(code(opposite(offset))),
            send_sem=send_sem.at[at], recv_sem=recv_sem.at[at],
            device_id=(peers[k],), device_id_type=MESH,
        ).start()

    def send(source, landing, at, first=0, last=N - 1):
        for k in range(first, last):
            send_one(source, landing, at, k)

    def received(ref, at):
        pltpu.make_async_copy(ref, ref, recv_sem.at[at]).wait()

    def sent(ref, at):
        pltpu.make_async_copy(ref, ref, send_sem.at[at]).wait()

    one_row = pl.ds(0, N - 1)
    far_rows = pl.ds(0, FAR)
    rest_rows = pl.ds(0, N - 1 - FAR)
    send(lambda p: req_out.at[p : p + 1], lambda m: req_in.at[m : m + 1], 0)

    for load in loads:
        load.wait()
    to_smem.wait()

    def put(pair, tile, at):
        high, low = halves(tile.T)
        weights[pair, 0:B, at * B : (at + 1) * B] = high
        weights[pair, B:, at * B : (at + 1) * B] = low

    def in_order(at):
        return raw[jnp.minimum(jnp.maximum(perm_smem[0, at], 0), TD - 1)]

    for pair in range(HALF):
        put(pair, in_order(2 * pair), 0)
        put(pair, in_order(2 * pair + 1), 1)
    for pair in range(RB // 2):
        put(HALF + pair, raw_diag[2 * pair], 0)
        put(HALF + pair, raw_diag[2 * pair + 1], 1)

    rows16 = iota((16, B), 0)

    def tile_products(high, low, first_pair, pairs, between=lambda: None):
        lhs = jnp.concatenate(
            [jnp.concatenate([high, high], axis=1), jnp.concatenate([low, low], axis=1)], axis=0
        )
        out = jnp.zeros((16, B), F32)
        for i in range(pairs):
            got = dot(lhs, weights[first_pair + i])
            between()
            got = got[0:16] + got[16:32]
            out = jnp.where(
                rows16 == 2 * i, got[:, 0:B], jnp.where(rows16 == 2 * i + 1, got[:, B:], out)
            )
        return out

    def block_products(picked, first_pair, between=lambda: None):
        return tile_products(picked[:, 0:B], picked[:, B:], first_pair, 8, between)

    def send_push(at):
        send(
            lambda p: xp_out.at[at, 2, p : p + 1], lambda m: xp_in.at[at, 2, m : m + 1], 4 + at
        )

    def send_x(at):
        planes = slice(0, 2) if at else slice(0, 1)
        send(
            lambda p: xp_out.at[at, planes, p : p + 1],
            lambda m: x_far.at[at, planes, FAR_CODES.index(m) : FAR_CODES.index(m) + 1],
            8 + at, 0, FAR,
        )
        left = iter(range(FAR, N - 1))

        def more(count):
            for k in itertools.islice(left, count):
                send_one(
                    lambda p: xp_out.at[at, planes, p : p + 1],
                    lambda m: xp_in.at[at, planes, m : m + 1], 1 + at, k,
                )

        return more

    def push(high, low, at, between=lambda: None, last=lambda: None):
        picked = dot(oh_cols[...], jnp.concatenate([high, low], axis=1)).astype(BF16)
        for b in range(3):
            products[16 * b : 16 * b + 16] = block_products(
                picked[16 * b : 16 * b + 16], 8 * b, between
            )
        last()
        p_high, p_low = halves(products[...])
        xp_out[at, 2] = dot(oh_push_out[...], jnp.concatenate([p_high, p_low], axis=0))

    def make_x(vector, high, low, dots_row, at):
        rest = (vector - high.astype(F32) - low.astype(F32)).astype(BF16)
        stacked = jnp.concatenate([high, low, rest], axis=0)
        xp_out[at, 0] = dot(oh_fetch_out[:, 0:HALF], stacked)
        if at:
            xp_out[at, 1] = jnp.broadcast_to(dots_row, (B, B))

    def finish(vector, high, low, at, reduced, images):
        planes = slice(0, 2) if at else slice(0, 1)
        products[TD : TD + 16] = tile_products(high, low, HALF, RB // 2)
        received(xp_in.at[at, planes, rest_rows], 1 + at)
        near = jnp.concatenate(halves(xp_in[at, 0]), axis=1)
        picked = dot(oh_fetch_in[0:32, 0:B], near).astype(BF16)
        for b in range(2):
            products[HALF + 16 * b : HALF + 16 * b + 16] = block_products(
                picked[16 * b : 16 * b + 16], 24 + 8 * b
            )
        received(x_far.at[at, planes, far_rows], 8 + at)
        far = jnp.concatenate(halves(x_far[at, 0]), axis=1)
        picked = dot(oh_fetch_in[32:48, 0:B], near) + dot(oh_fetch_in[32:48, B : B + 16], far)
        products[HALF + 32 : TD] = block_products(picked.astype(BF16), 40)
        p_high, p_low = halves(products[...])
        here = mass * vector + dot(oh_local[...], jnp.concatenate([p_high, p_low], axis=0))
        sums = reduced()
        norm = sums[-1]
        for term, image in zip(sums, images):
            norm = norm - term * term
            here = here - term * image
        norm = jnp.sqrt(norm)
        scale = 1.0 / norm
        here = here * scale
        received(xp_in.at[at, 2, one_row], 4 + at)
        p_high, p_low = halves(xp_in[at, 2])
        image = here + scale * dot(oh_push_in[...], jnp.concatenate([p_high, p_low], axis=0))
        return sums[:-1], norm, scale, image

    def packed(values):
        row = jnp.zeros((1, B), F32)
        for i, value in enumerate(values):
            row = jnp.where(lane_row == i, value, row)
        return row

    def unpacked(row, count):
        return [
            jnp.sum(jnp.where(lane_row == i, row, 0.0), axis=1, keepdims=True)
            for i in range(count)
        ]

    u_high, u_low = halves(u0)
    push(u_high, u_low, 0)
    received(req_in.at[one_row], 0)
    req = req_in[...]
    asked = req[:, 0:1].astype(jnp.int32) - 1
    oh_fetch_out[...] = jnp.where((asked == slot) & (lanes < 48), 1.0, 0.0).astype(BF16)
    make_x(u0, u_high, u_low, None, 0)
    send_x(0)(N)
    send_push(0)
    landing = req[:, 1:2].astype(jnp.int32) - 1
    into = jnp.where(landing == lanes, 1.0, 0.0).T[0:16].astype(BF16)
    oh_push_in[:, 0:B] = into
    oh_push_in[:, B:] = into
    beta_row = jnp.where(lane_row == 2, jnp.sum(req, axis=0, keepdims=True), 0.0)
    beta_square = jnp.sum(beta_row, axis=1, keepdims=True) + beta_part
    _, beta, scale, w0 = finish(u0, u_high, u_low, 0, lambda: [beta_square], [])
    v0 = u0 * scale

    def apply_with_dots(vector, others, images, at):
        row = packed([total(other * vector) for other in others] + [total(vector * vector)])
        high, low = halves(vector)
        make_x(vector, high, low, row, at)
        more = send_x(at)
        push(high, low, at, lambda: more(4), lambda: more(N))
        send_push(at)

        def reduced():
            sums = jnp.sum(xp_in[at, 1], axis=0, keepdims=True) + row
            sums = sums + jnp.sum(x_far[at, 1], axis=0, keepdims=True)
            return unpacked(sums, len(others) + 1)

        return finish(vector, high, low, at, reduced, images)

    (h00,), h10, scale, w1 = apply_with_dots(w0, [v0], [w0], 1)
    v1 = (w0 - h00 * v0) * scale
    (h01, h11), h21, scale, w2 = apply_with_dots(w1, [v0, v1], [w0, w1], 2)
    v2 = (w1 - h01 * v0 - h11 * v1) * scale

    row = packed([total(v0 * w2), total(v1 * w2), total(v2 * w2), total(w2 * w2)])
    f_out[...] = jnp.broadcast_to(row, (8, B))
    send(lambda p: f_out.at[0:1], lambda m: f_in.at[m : m + 1], 7)
    h00, h11 = h00 + SHIFT, h11 + SHIFT
    l00_inv = 1.0 / jnp.sqrt(h00 * h00 + h10 * h10)
    l10 = (h01 * h00 + h11 * h10) * l00_inv
    l11_inv = 1.0 / jnp.sqrt(h01 * h01 + h11 * h11 + h21 * h21 - l10 * l10)
    t0 = beta * h00 * l00_inv
    t1 = (beta * h01 - l10 * t0) * l11_inv

    sent(req_out.at[one_row], 0)
    for at in range(3):
        planes = slice(0, 2) if at else slice(0, 1)
        sent(xp_in.at[at, planes, rest_rows], 1 + at)
        sent(x_far.at[at, planes, far_rows], 8 + at)
        sent(xp_in.at[at, 2, one_row], 4 + at)
    received(f_in.at[one_row], 7)
    sums = jnp.sum(f_in[...], axis=0, keepdims=True) + row
    h02, h12, h22, square = unpacked(sums, 4)
    h32_square = square - h02 * h02 - h12 * h12 - h22 * h22
    h22 = h22 + SHIFT
    l20 = (h02 * h00 + h12 * h10) * l00_inv
    l21 = (h02 * h01 + h12 * h11 + h22 * h21 - l20 * l10) * l11_inv
    pivot = h02 * h02 + h12 * h12 + h22 * h22 + h32_square - l20 * l20 - l21 * l21
    m2 = (beta * h02 - l20 * t0 - l21 * t1) / pivot
    m1 = (t1 - l21 * m2) * l11_inv
    m0 = (t0 - l10 * m1 - l20 * m2) * l00_inv
    update = m0 * v0 + m1 * v1 + m2 * v2
    out_ref[...] = update[0:RB]

    sent(f_in.at[one_row], 7)


def on_device(defect, mass, block_diag, coupling, tile_rows, tile_cols):
    vmem = pl.BlockSpec(memory_space=pltpu.VMEM)
    hbm = pl.BlockSpec(memory_space=pl.ANY)
    return pl.pallas_call(
        kernel,
        out_shape=pltpu.VMEM(defect.shape, F32),
        in_specs=[hbm] * 6,
        out_specs=vmem,
        scratch_shapes=[
            pltpu.VMEM((2, 1, TD), jnp.int32),
            pltpu.VMEM((2, 16, B), F32),
            pltpu.VMEM((TD, B, B), F32),
            pltpu.VMEM((RB, B, B), F32),
            pltpu.VMEM((54, 2 * B, 2 * B), BF16),
            pltpu.VMEM((8, B), jnp.int32),
            pltpu.VMEM((1, B), jnp.int32),
            pltpu.SMEM((1, B), jnp.int32),
            pltpu.VMEM((B, B), F32),
            pltpu.VMEM((B, B), BF16),
            pltpu.VMEM((16, 2 * B), BF16),
            pltpu.VMEM((HALF, 16), BF16),
            pltpu.VMEM((B, 2 * B), BF16),
            pltpu.VMEM((16, 2 * B), BF16),
            pltpu.VMEM((HALF, 2 * B), BF16),
            pltpu.VMEM((N, B), F32),
            pltpu.VMEM((N, B), F32),
            pltpu.VMEM((3, 3, N, B), F32),
            pltpu.VMEM((3, 3, N, B), F32),
            pltpu.VMEM((3, 2, 16, B), F32),
            pltpu.VMEM((8, B), F32),
            pltpu.VMEM((N, B), F32),
            pltpu.SemaphoreType.DMA((7,)),
            pltpu.SemaphoreType.DMA((4,)),
            pltpu.SemaphoreType.DMA,
            pltpu.SemaphoreType.DMA((11,)),
            pltpu.SemaphoreType.DMA((11,)),
        ],
        compiler_params=pltpu.CompilerParams(collective_id=0, has_side_effects=True),
    )(
        defect, mass, block_diag, coupling,
        tile_rows.reshape(1, TD), tile_cols.reshape(1, TD),
    )


def solution(mesh):
    return jax.shard_map(
        on_device,
        mesh=mesh,
        in_specs=(
            P("blk", None),
            P("blk", None),
            P("blk", None, None),
            P("blk", None, None),
            P("blk"),
            P("blk"),
        ),
        out_specs=P("blk", None),
        check_vma=False,
    )
```

```python
import itertools

import jax
import jax.numpy as jnp
from jax import lax
from jax.experimental import pallas as pl
from jax.experimental.pallas import tpu as pltpu
from jax.sharding import PartitionSpec as P

N = 128
RB = 12
TD = 96
HALF = 48
B = 128
SHIFT = 1.5
F32 = jnp.float32
BF16 = jnp.bfloat16
MESH = pl.DeviceIdType.MESH


def distance(offset):
    return sum(min(step, 4 - step) for step in offset[:3])


def mixed(offset):
    at = offset[0] * 32 + offset[1] * 8 + offset[2] * 2 + offset[3]
    return at * 37 % 128


OFFSETS = sorted(
    (o for o in itertools.product(range(4), range(4), range(4), range(2)) if any(o)),
    key=lambda o: (-distance(o), mixed(o)),
)


def code(offset):
    return offset[0] * 32 + offset[1] * 8 + offset[2] * 2 + offset[3]


def opposite(offset):
    return tuple((4 - step) % 4 for step in offset[:3]) + (offset[3],)


FAR = 14
FAR_CODES = [code(o) for o in OFFSETS[:FAR]]


def dot(a, b):
    return lax.dot_general(a, b, (((1,), (0,)), ((), ())), preferred_element_type=F32)


def dot_nt(a, b):
    return lax.dot_general(a, b, (((1,), (1,)), ((), ())), preferred_element_type=F32)


def iota(shape, dim):
    return lax.broadcasted_iota(jnp.int32, shape, dim)


def halves(x):
    high = x.astype(BF16)
    low = (x - high.astype(F32)).astype(BF16)
    return high, low


def total(x):
    return jnp.sum(jnp.sum(x, axis=0, keepdims=True), axis=1, keepdims=True)


def divided_by_rb(x):
    return lax.shift_right_logical(x * 21846, 18)


def kernel(
    defect_hbm, mass_hbm, diag_hbm, coup_hbm, rows_hbm, cols_hbm, out_ref,
    indices, vectors, raw, raw_diag, weights, index_rows, perm_vmem, perm_smem,
    products, oh_fetch_out, oh_push_in, oh_cols, oh_push_out, oh_local,
    oh_fetch_in, req_out, req_in, xp_out, xp_in, x_far, f_out, f_in,
    load_sem, small_sem, perm_sem, send_sem, recv_sem,
):
    me = lax.axis_index("blk")
    y, z, x, c = me // 32, (me // 8) % 4, (me // 2) % 4, me % 2
    y_part = [((y + d) % 4) * 32 for d in range(4)]
    z_part = [((z + d) % 4) * 8 for d in range(4)]
    x_part = [((x + d) % 4) * 2 for d in range(4)]
    c_part = [(c + d) % 2 for d in range(2)]
    yz = [[y_part[a] + z_part[b] for b in range(4)] for a in range(4)]
    xc = [[x_part[a] + c_part[b] for b in range(2)] for a in range(4)]
    peers = [yz[o[0]][o[1]] + xc[o[2]][o[3]] for o in OFFSETS]

    small_loads = [
        pltpu.make_async_copy(rows_hbm, indices.at[0], small_sem.at[0]),
        pltpu.make_async_copy(cols_hbm, indices.at[1], small_sem.at[1]),
        pltpu.make_async_copy(defect_hbm, vectors.at[0, 0:RB], small_sem.at[2]),
        pltpu.make_async_copy(mass_hbm, vectors.at[1, 0:RB], small_sem.at[3]),
    ]
    loads = [
        pltpu.make_async_copy(
            coup_hbm.at[pl.ds(16 * i, 16)], raw.at[pl.ds(16 * i, 16)], load_sem.at[i]
        )
        for i in range(6)
    ]
    loads.append(pltpu.make_async_copy(diag_hbm, raw_diag, load_sem.at[6]))
    for load in small_loads + loads:
        load.start()

    nothing = jnp.zeros((1, B), F32)
    req_in[0:1] = nothing
    f_in[0:1] = nothing
    for at in range(3):
        xp_in[at, 0:2] = jnp.zeros((2, N, B), F32)
        xp_in[at, 2, 0:1] = nothing
    x_far[...] = jnp.zeros_like(x_far)

    barrier = pltpu.get_barrier_semaphore()
    for peer in peers:
        pl.semaphore_signal(barrier, inc=1, device_id=(peer,), device_id_type=MESH)

    lane_row = iota((1, B), 1)
    lanes = iota((B, B), 1)
    subs = iota((B, B), 0)
    products[...] = jnp.zeros_like(products)
    for load in small_loads:
        load.wait()
    index_rows[...] = jnp.zeros_like(index_rows)
    index_rows[0:1, 0:TD] = indices[0]
    index_rows[1:2, 0:TD] = indices[1]
    rows = index_rows[0:1, :]
    cols = index_rows[1:2, :]
    row_owner = divided_by_rb(rows)
    col_owner = divided_by_rb(cols)

    def hop(d):
        return jnp.where(d == 3, 1, d)

    def relative(owner):
        dy = (lax.shift_right_logical(owner, 5) - y) & 3
        dz = (lax.shift_right_logical(owner, 3) - z) & 3
        dx = (lax.shift_right_logical(owner, 1) - x) & 3
        dc = (owner + c) & 1
        return dy * 32 + dz * 8 + dx * 2 + dc, hop(dy) + hop(dz) + hop(dx) >= 5

    row_local = rows - row_owner * RB
    col_local = cols - col_owner * RB
    valid = lane_row < TD
    push = valid & (row_owner != me)
    fetch = valid & (row_owner == me)
    destination, is_far = relative(jnp.where(push, row_owner, col_owner))
    sub8 = iota((16, B), 0)
    kinds = [push & is_far, push & ~is_far, fetch & ~is_far, fetch & is_far]
    members = jnp.zeros((16, B), F32)
    for at, kind in enumerate(kinds):
        members = jnp.where((sub8 == at) & kind, 1.0, members)
    counts = jnp.sum(members, axis=1, keepdims=True)
    ranks = dot(members.astype(BF16), jnp.where(subs < lanes, 1.0, 0.0).astype(BF16))
    starts = [0.0, counts[0:1], HALF * 1.0, counts[2:3] + HALF]
    position = jnp.full((1, B), 1000.0, F32)
    for at, kind in enumerate(kinds):
        position = jnp.where(kind, ranks[at : at + 1] + starts[at], position)
    position = position.astype(jnp.int32)
    order = jnp.where(position == subs, 1.0, 0.0).astype(BF16)

    def as_f(v):
        return v.astype(F32)

    wanted = jnp.where(fetch, as_f(col_local) + 1.0, 0.0)
    target = jnp.where(push, as_f(row_local) + 1.0, 0.0)
    table = jnp.zeros((B, B), F32)
    for at, value in enumerate(
        (wanted, target, as_f(destination), as_f(col_local), as_f(row_local), as_f(lane_row))
    ):
        table = jnp.where(subs == at, value, table)
    table = table.astype(BF16)
    by_lane = dot_nt(table, order)
    by_sub = dot_nt(order, table)
    dest_lane = by_lane[2:3].astype(jnp.int32)
    row_local_lane = by_lane[4:5].astype(jnp.int32)
    perm_vmem[...] = by_lane[5:6].astype(jnp.int32)
    to_smem = pltpu.make_async_copy(perm_vmem, perm_smem, perm_sem)
    to_smem.start()

    sends_to = jnp.where((dest_lane == subs) & (lanes < TD), 1.0, 0.0)
    push_out = jnp.where(lanes < HALF, sends_to, 0.0).astype(BF16)
    oh_push_out[:, 0:B] = push_out
    oh_push_out[:, B:] = push_out
    slot = lanes % 16
    dest_sub = by_sub[HALF:TD, 2:3].astype(jnp.int32)
    oh_fetch_in[:, 0:B] = jnp.where(dest_sub == lanes[0:HALF], 1.0, 0.0).astype(BF16)
    far_codes = jnp.full((1, B), -1, jnp.int32)
    for at, value in enumerate(FAR_CODES):
        far_codes = jnp.where(lane_row == at, value, far_codes)
    oh_fetch_in[:, B:] = jnp.where(dest_sub == far_codes, 1.0, 0.0).astype(BF16)
    col_local_sub = by_sub[0:HALF, 3:4].astype(jnp.int32)
    oh_cols[...] = jnp.where(col_local_sub == iota((HALF, 16), 1), 1.0, 0.0).astype(BF16)
    lanes16 = iota((16, B), 1)
    local_target = jnp.where(
        (lanes16 >= HALF) & (lanes16 < TD),
        row_local_lane,
        jnp.where((lanes16 >= TD) & (lanes16 < TD + RB), lanes16 - TD, -1),
    )
    local = jnp.where(local_target == sub8, 1.0, 0.0).astype(BF16)
    oh_local[:, 0:B] = local
    oh_local[:, B:] = local

    own_rows = iota((16, B), 0) < RB
    u0 = jnp.where(own_rows, -vectors[0], 0.0)
    mass = jnp.where(own_rows, vectors[1] - SHIFT, 0.0)
    beta_part = total(u0 * u0)
    message = dot(sends_to.astype(BF16), by_sub.astype(BF16))
    req_out[...] = jnp.where(lanes < 2, message, jnp.where(lanes == 2, beta_part, 0.0))

    pl.semaphore_wait(barrier, N - 1)

    def send_one(source, landing, at, k):
        offset = OFFSETS[k]
        pltpu.make_async_remote_copy(
            src_ref=source(code(offset)), dst_ref=landing(code(opposite(offset))),
            send_sem=send_sem.at[at], recv_sem=recv_sem.at[at],
            device_id=(peers[k],), device_id_type=MESH,
        ).start()

    def send(source, landing, at, first=0, last=N - 1):
        for k in range(first, last):
            send_one(source, landing, at, k)

    def received(ref, at):
        pltpu.make_async_copy(ref, ref, recv_sem.at[at]).wait()

    def sent(ref, at):
        pltpu.make_async_copy(ref, ref, send_sem.at[at]).wait()

    one_row = pl.ds(0, N - 1)
    far_rows = pl.ds(0, FAR)
    rest_rows = pl.ds(0, N - 1 - FAR)
    send(lambda p: req_out.at[p : p + 1], lambda m: req_in.at[m : m + 1], 0)

    for load in loads:
        load.wait()
    to_smem.wait()

    def put(pair, tile, at):
        high, low = halves(tile.T)
        weights[pair, 0:B, at * B : (at + 1) * B] = high
        weights[pair, B:, at * B : (at + 1) * B] = low

    def in_order(at):
        return raw[jnp.minimum(jnp.maximum(perm_smem[0, at], 0), TD - 1)]

    for pair in range(HALF):
        put(pair, in_order(2 * pair), 0)
        put(pair, in_order(2 * pair + 1), 1)
    for pair in range(RB // 2):
        put(HALF + pair, raw_diag[2 * pair], 0)
        put(HALF + pair, raw_diag[2 * pair + 1], 1)

    rows16 = iota((16, B), 0)

    def tile_products(high, low, first_pair, pairs, between=lambda: None):
        lhs = jnp.concatenate(
            [jnp.concatenate([high, high], axis=1), jnp.concatenate([low, low], axis=1)], axis=0
        )
        out = jnp.zeros((16, B), F32)
        for i in range(pairs):
            got = dot(lhs, weights[first_pair + i])
            between()
            got = got[0:16] + got[16:32]
            out = jnp.where(
                rows16 == 2 * i, got[:, 0:B], jnp.where(rows16 == 2 * i + 1, got[:, B:], out)
            )
        return out

    def block_products(picked, first_pair, between=lambda: None):
        return tile_products(picked[:, 0:B], picked[:, B:], first_pair, 8, between)

    def send_push(at):
        send(
            lambda p: xp_out.at[at, 2, p : p + 1], lambda m: xp_in.at[at, 2, m : m + 1], 4 + at
        )

    def send_x(at):
        planes = slice(0, 2) if at else slice(0, 1)
        send(
            lambda p: xp_out.at[at, planes, p : p + 1],
            lambda m: x_far.at[at, planes, FAR_CODES.index(m) : FAR_CODES.index(m) + 1],
            8 + at, 0, FAR,
        )
        left = iter(range(FAR, N - 1))

        def more(count):
            for k in itertools.islice(left, count):
                send_one(
                    lambda p: xp_out.at[at, planes, p : p + 1],
                    lambda m: xp_in.at[at, planes, m : m + 1], 1 + at, k,
                )

        return more

    def push(high, low, at, between=lambda: None):
        picked = dot(oh_cols[...], jnp.concatenate([high, low], axis=1)).astype(BF16)
        for b in range(3):
            products[16 * b : 16 * b + 16] = block_products(
                picked[16 * b : 16 * b + 16], 8 * b, between
            )
        p_high, p_low = halves(products[...])
        xp_out[at, 2] = dot(oh_push_out[...], jnp.concatenate([p_high, p_low], axis=0))

    def make_x(vector, high, low, dots_row, at):
        rest = (vector - high.astype(F32) - low.astype(F32)).astype(BF16)
        stacked = jnp.concatenate([high, low, rest], axis=0)
        xp_out[at, 0] = dot(oh_fetch_out[:, 0:HALF], stacked)
        if at:
            xp_out[at, 1] = jnp.broadcast_to(dots_row, (B, B))

    def finish(vector, high, low, at, reduced, images):
        planes = slice(0, 2) if at else slice(0, 1)
        products[TD : TD + 16] = tile_products(high, low, HALF, RB // 2)
        received(xp_in.at[at, planes, rest_rows], 1 + at)
        near = jnp.concatenate(halves(xp_in[at, 0]), axis=1)
        picked = dot(oh_fetch_in[0:32, 0:B], near).astype(BF16)
        for b in range(2):
            products[HALF + 16 * b : HALF + 16 * b + 16] = block_products(
                picked[16 * b : 16 * b + 16], 24 + 8 * b
            )
        received(x_far.at[at, planes, far_rows], 8 + at)
        far = jnp.concatenate(halves(x_far[at, 0]), axis=1)
        picked = dot(oh_fetch_in[32:48, 0:B], near) + dot(oh_fetch_in[32:48, B : B + 16], far)
        products[HALF + 32 : TD] = block_products(picked.astype(BF16), 40)
        p_high, p_low = halves(products[...])
        here = mass * vector + dot(oh_local[...], jnp.concatenate([p_high, p_low], axis=0))
        sums = reduced()
        norm = sums[-1]
        for term, image in zip(sums, images):
            norm = norm - term * term
            here = here - term * image
        norm = jnp.sqrt(norm)
        scale = 1.0 / norm
        here = here * scale
        received(xp_in.at[at, 2, one_row], 4 + at)
        p_high, p_low = halves(xp_in[at, 2])
        image = here + scale * dot(oh_push_in[...], jnp.concatenate([p_high, p_low], axis=0))
        return sums[:-1], norm, scale, image

    def packed(values):
        row = jnp.zeros((1, B), F32)
        for i, value in enumerate(values):
            row = jnp.where(lane_row == i, value, row)
        return row

    def unpacked(row, count):
        return [
            jnp.sum(jnp.where(lane_row == i, row, 0.0), axis=1, keepdims=True)
            for i in range(count)
        ]

    u_high, u_low = halves(u0)
    push(u_high, u_low, 0)
    received(req_in.at[one_row], 0)
    req = req_in[...]
    asked = req[:, 0:1].astype(jnp.int32) - 1
    oh_fetch_out[...] = jnp.where((asked == slot) & (lanes < 48), 1.0, 0.0).astype(BF16)
    make_x(u0, u_high, u_low, None, 0)
    send_x(0)(N)
    send_push(0)
    landing = req[:, 1:2].astype(jnp.int32) - 1
    into = jnp.where(landing == lanes, 1.0, 0.0).T[0:16].astype(BF16)
    oh_push_in[:, 0:B] = into
    oh_push_in[:, B:] = into
    beta_row = jnp.where(lane_row == 2, jnp.sum(req, axis=0, keepdims=True), 0.0)
    beta_square = jnp.sum(beta_row, axis=1, keepdims=True) + beta_part
    _, beta, scale, w0 = finish(u0, u_high, u_low, 0, lambda: [beta_square], [])
    v0 = u0 * scale

    def apply_with_dots(vector, others, images, at):
        row = packed([total(other * vector) for other in others] + [total(vector * vector)])
        high, low = halves(vector)
        make_x(vector, high, low, row, at)
        more = send_x(at)
        more(20)
        push(high, low, at, lambda: more(4))
        more(N)
        send_push(at)

        def reduced():
            sums = jnp.sum(xp_in[at, 1], axis=0, keepdims=True) + row
            sums = sums + jnp.sum(x_far[at, 1], axis=0, keepdims=True)
            return unpacked(sums, len(others) + 1)

        return finish(vector, high, low, at, reduced, images)

    (h00,), h10, scale, w1 = apply_with_dots(w0, [v0], [w0], 1)
    v1 = (w0 - h00 * v0) * scale
    (h01, h11), h21, scale, w2 = apply_with_dots(w1, [v0, v1], [w0, w1], 2)
    v2 = (w1 - h01 * v0 - h11 * v1) * scale

    row = packed([total(v0 * w2), total(v1 * w2), total(v2 * w2), total(w2 * w2)])
    f_out[...] = jnp.broadcast_to(row, (8, B))
    send(lambda p: f_out.at[0:1], lambda m: f_in.at[m : m + 1], 7)
    h00, h11 = h00 + SHIFT, h11 + SHIFT
    l00_inv = 1.0 / jnp.sqrt(h00 * h00 + h10 * h10)
    l10 = (h01 * h00 + h11 * h10) * l00_inv
    l11_inv = 1.0 / jnp.sqrt(h01 * h01 + h11 * h11 + h21 * h21 - l10 * l10)
    t0 = beta * h00 * l00_inv
    t1 = (beta * h01 - l10 * t0) * l11_inv

    sent(req_out.at[one_row], 0)
    for at in range(3):
        planes = slice(0, 2) if at else slice(0, 1)
        sent(xp_in.at[at, planes, rest_rows], 1 + at)
        sent(x_far.at[at, planes, far_rows], 8 + at)
        sent(xp_in.at[at, 2, one_row], 4 + at)
    received(f_in.at[one_row], 7)
    sums = jnp.sum(f_in[...], axis=0, keepdims=True) + row
    h02, h12, h22, square = unpacked(sums, 4)
    h32_square = square - h02 * h02 - h12 * h12 - h22 * h22
    h22 = h22 + SHIFT
    l20 = (h02 * h00 + h12 * h10) * l00_inv
    l21 = (h02 * h01 + h12 * h11 + h22 * h21 - l20 * l10) * l11_inv
    pivot = h02 * h02 + h12 * h12 + h22 * h22 + h32_square - l20 * l20 - l21 * l21
    m2 = (beta * h02 - l20 * t0 - l21 * t1) / pivot
    m1 = (t1 - l21 * m2) * l11_inv
    m0 = (t0 - l10 * m1 - l20 * m2) * l00_inv
    update = m0 * v0 + m1 * v1 + m2 * v2
    out_ref[...] = update[0:RB]

    sent(f_in.at[one_row], 7)


def on_device(defect, mass, block_diag, coupling, tile_rows, tile_cols):
    vmem = pl.BlockSpec(memory_space=pltpu.VMEM)
    hbm = pl.BlockSpec(memory_space=pl.ANY)
    return pl.pallas_call(
        kernel,
        out_shape=pltpu.VMEM(defect.shape, F32),
        in_specs=[hbm] * 6,
        out_specs=vmem,
        scratch_shapes=[
            pltpu.VMEM((2, 1, TD), jnp.int32),
            pltpu.VMEM((2, 16, B), F32),
            pltpu.VMEM((TD, B, B), F32),
            pltpu.VMEM((RB, B, B), F32),
            pltpu.VMEM((54, 2 * B, 2 * B), BF16),
            pltpu.VMEM((8, B), jnp.int32),
            pltpu.VMEM((1, B), jnp.int32),
            pltpu.SMEM((1, B), jnp.int32),
            pltpu.VMEM((B, B), F32),
            pltpu.VMEM((B, B), BF16),
            pltpu.VMEM((16, 2 * B), BF16),
            pltpu.VMEM((HALF, 16), BF16),
            pltpu.VMEM((B, 2 * B), BF16),
            pltpu.VMEM((16, 2 * B), BF16),
            pltpu.VMEM((HALF, 2 * B), BF16),
            pltpu.VMEM((N, B), F32),
            pltpu.VMEM((N, B), F32),
            pltpu.VMEM((3, 3, N, B), F32),
            pltpu.VMEM((3, 3, N, B), F32),
            pltpu.VMEM((3, 2, 16, B), F32),
            pltpu.VMEM((8, B), F32),
            pltpu.VMEM((N, B), F32),
            pltpu.SemaphoreType.DMA((7,)),
            pltpu.SemaphoreType.DMA((4,)),
            pltpu.SemaphoreType.DMA,
            pltpu.SemaphoreType.DMA((11,)),
            pltpu.SemaphoreType.DMA((11,)),
        ],
        compiler_params=pltpu.CompilerParams(collective_id=0, has_side_effects=True),
    )(
        defect, mass, block_diag, coupling,
        tile_rows.reshape(1, TD), tile_cols.reshape(1, TD),
    )


def solution(mesh):
    return jax.shard_map(
        on_device,
        mesh=mesh,
        in_specs=(
            P("blk", None),
            P("blk", None),
            P("blk", None, None),
            P("blk", None, None),
            P("blk"),
            P("blk"),
        ),
        out_specs=P("blk", None),
        check_vma=False,
    )
```
